32 devices in a mesh: groups: 2 (over y), grid: 4 (over z), row: 2 (over core), rep: 2 (over x).
Axes of the slice: x: 2, y: 2, z: 4, core: 2. Of those that a mesh axis runs over, the one named last changes fastest.
Arguments:
- tokens: bfloat16 [1024, 4096], P(('groups', 'grid', 'rep'), 'row'), parts along dimension 0, may hold values from -40 to 40
- target_tokens: int32 [1024], P('groups'), parts along dimension 0, may hold values from 0 to 31999
- gate_weight: bfloat16 [4096, 14336], P(('row', 'rep'), 'grid'), may hold values from -0.09375 to 0.09375
- up_weight: bfloat16 [4096, 14336], P(('row', 'rep'), 'grid'), may hold values from -0.09375 to 0.09375
- down_weight: bfloat16 [14336, 4096], P('grid', ('row', 'rep')), may hold values from -0.046875 to 0.046875
- norm_gain: float32 [4096], P('row'), may hold values from 0.5 to 1.5
- vocab_weight: bfloat16 [4096, 32000], P('row', ('grid', 'rep')), may hold values from -6 to 6
Outputs:
- mixed: bfloat16 [1024, 4096], P(('groups', 'grid', 'rep'), 'row'), parts along dimension 0
- logprob: float32 [1024], P(('groups', 'grid', 'rep')), parts along dimension 0
The draws below stay inside these ranges and needn't reach their ends.
There are 2 independent parts, one for each index of `groups`. The reference program is written for one: setup_inputs(seed, part) draws one part's arguments, and reference() takes and returns one part's arrays. A program takes and returns all parts, laid end to end along the dimension named above; an argument that names none is the same for every part. Nothing has to cross between parts.
All inputs are finite; a program needn't handle non-finite values.
Results may differ from the reference program's by a relative error of at most 0.0046.
Values may be sent and summed in bfloat16 or wider, within the bound.
A program may use at most 128 MiB of HBM per device.

```python
import math
import jax
import jax.numpy as jnp
import numpy as np
from jax import lax

D = 4096
FF = 14336
V = 32000
TOKENS = 512


def draw_tokens(key, part):
    key_rows = jax.random.fold_in(key, 0)
    key_cols = jax.random.fold_in(key, 1)
    key_base = jax.random.fold_in(key, 2)
    key_pick = jax.random.fold_in(key, 4)
    key_level = jax.random.fold_in(key, 5)
    key_noise = jax.random.fold_in(key, 6)
    key_mix = jax.random.fold_in(key, 7)
    row_scale = jnp.exp(jax.random.uniform(key_rows, (TOKENS, 1), minval=math.log(0.4), maxval=math.log(4.0)))
    column_ramp = jnp.arange(D, dtype=jnp.float32) / D
    column_scale = 0.5 * jnp.exp(math.log(3.0) * column_ramp + jax.random.uniform(key_cols, (D,), minval=-0.2, maxval=0.2))
    base_draw = jnp.clip(jax.random.normal(key_base, (TOKENS, D)), -5.5, 5.5)
    drawn = base_draw * row_scale * column_scale
    aligned_row = jax.random.randint(key_pick, (TOKENS, 1), 0, 12) == 0
    level = jax.random.uniform(key_level, (TOKENS, 1), minval=2.0, maxval=3.0)
    mix_share = jax.random.uniform(key_mix, (TOKENS, 1), minval=0.15, maxval=2.0)
    noise = jnp.clip(jax.random.normal(key_noise, (TOKENS, D)), -5.0, 5.0)
    aligned = level * (1.0 + mix_share * noise)
    return jnp.clip(jnp.where(aligned_row, aligned, drawn), -40.0, 40.0).astype(jnp.bfloat16)


def draw_vocab_weight(key, part):
    key_base, key_scale, key_heavy, key_pair = jax.random.split(key, 4)
    column_ramp = jnp.arange(V, dtype=jnp.float32) / V
    column_scale = (2.5 + column_ramp + jax.random.uniform(key_scale, (V,), minval=-0.3, maxval=0.3)) / math.sqrt(D)
    base_draw = jnp.clip(jax.random.normal(key_base, (D, V)), -5.0, 5.0) * column_scale
    heavy_level = 320.0 / D
    heavy_draw = heavy_level * (1.0 + 0.15 * jnp.clip(jax.random.normal(key_heavy, (D, V)), -4.0, 4.0))
    partner_draw = jnp.roll(heavy_draw, 1, axis=1) + jnp.clip(jax.random.normal(key_pair, (D, V)), -5.0, 5.0) * (1.5 / math.sqrt(D))
    position = jnp.arange(V) % (V // 4)
    base_draw = jnp.where(position == 0, heavy_draw, jnp.where(position == 1, partner_draw, base_draw))
    return jnp.clip(base_draw, -6.0, 6.0).astype(jnp.bfloat16)


def set_ends(drawn, rng, least, high):
    dims = drawn.shape
    spot = [jax.random.randint(jax.random.fold_in(rng, axis), (), 0, dims[axis]) for axis in range(len(dims))]
    drawn = drawn.at[tuple(spot)].set(least)
    longest = dims.index(max(dims))
    spot[longest] = (spot[longest] + 1) % dims[longest]
    return drawn.at[tuple(spot)].set(high)


def steps_of(own_key, extent, cuts, low, high):
    def one(axis_at, blocks):
        heights = jax.random.uniform(jax.random.fold_in(jax.random.fold_in(own_key, 6), axis_at), (blocks,), jnp.float32, low / len(cuts), high / len(cuts))
        return jnp.repeat(jnp.exp(heights), extent[axis_at] // blocks).reshape((-1,) + (1,) * (len(extent) - axis_at - 1))

    loudness = one(*cuts[0])
    for cut in cuts[1:]:
        loudness = loudness * one(*cut)
    return loudness


def cumulative_ranks(amount, skew):
    portions = [(1 << 20) // math.isqrt(rank ** skew) + 1 for rank in range(1, amount + 1)]
    scale = 1 + sum(portions) // (1 << 30)
    return np.cumsum(np.array([max(1, weight // scale) for weight in portions]))


def ranked(stream_key, shape, count, lean):
    table = cumulative_ranks(count, lean)
    pick = jax.random.randint(jax.random.fold_in(stream_key, 1), shape, 0, int(table[count - 1]))
    standing = jnp.searchsorted(jnp.asarray(table, jnp.int32), pick, side="right")
    return jax.random.permutation(jax.random.fold_in(stream_key, 2), count)[standing].astype(jnp.int32)


def scatter_about(key, extent, scale, limit, cuts=(), kind=jnp.bfloat16):
    result = jax.random.normal(key, extent, jnp.float32) * scale
    if len(cuts) > 0:
        result = steps_of(key, extent, cuts, -0.22, 0.18) * result
    return jnp.clip(result, min=-limit, max=limit).astype(kind)


def setup_inputs(seed: int = 0, part: int = 0) -> dict:
    streams_of = jax.random.split(jax.random.key(seed), 8)
    part_keys = jax.random.split(jax.random.fold_in(streams_of[7], part), 8)
    tokens = draw_tokens(jax.random.fold_in(jax.random.fold_in(streams_of[7], part), 71), part)
    target_tokens = set_ends(ranked(part_keys[1], (TOKENS,), V, 2), jax.random.fold_in(part_keys[1], 3), 0, V - 1).astype(jnp.int32)
    gate_weight = scatter_about(streams_of[2], (D, FF), D ** -0.5, 0.09375, ((0, 4), (1, 4)))
    up_weight = scatter_about(streams_of[3], (D, FF), D ** -0.5, 0.09375, ((0, 4), (1, 4)))
    down_weight = scatter_about(streams_of[4], (FF, D), FF ** -0.5, 0.046875, ((0, 4), (1, 4)))
    norm_gain = jnp.clip(1.0 + 0.1 * jax.random.normal(streams_of[5], (D,), jnp.float32), 0.5, 1.5)
    vocab_weight = draw_vocab_weight(jax.random.fold_in(streams_of[7], 71), part)
    return {"tokens": tokens, "target_tokens": target_tokens, "gate_weight": gate_weight, "up_weight": up_weight, "down_weight": down_weight, "norm_gain": norm_gain, "vocab_weight": vocab_weight}


def reference(tokens, target_tokens, gate_weight, up_weight, down_weight, norm_gain, vocab_weight):
    gate_value = jnp.dot(tokens, gate_weight, preferred_element_type=jnp.float32)
    up_value = jnp.dot(tokens, up_weight, preferred_element_type=jnp.float32)
    hidden = (jax.nn.silu(gate_value) * up_value).astype(jnp.bfloat16)
    mixed_full = tokens.astype(jnp.float32) + jnp.dot(hidden, down_weight, preferred_element_type=jnp.float32)
    mixed = mixed_full.astype(jnp.bfloat16)
    held = lax.optimization_barrier(mixed).astype(jnp.float32)
    scale = lax.rsqrt(lax.optimization_barrier(jnp.sum(held * held, axis=1, keepdims=True)) / D + 1e-05)
    normed = (held * scale * norm_gain.astype(jnp.float32)).astype(jnp.bfloat16)
    logits = jnp.dot(normed, vocab_weight, preferred_element_type=jnp.float32)
    row_top = lax.optimization_barrier(jnp.max(logits, axis=1, keepdims=True))
    row_total = lax.optimization_barrier(jnp.sum(jnp.exp(logits - row_top), axis=1))
    picked = jnp.take_along_axis(logits, target_tokens.astype(jnp.int32)[:, None], axis=1)[:, 0]
    logprob = picked - row_top[:, 0] - jnp.log(row_total)
    return (mixed, logprob)
```

```python
import jax
import jax.numpy as jnp
from jax import lax
from jax.experimental import pallas as pl
from jax.experimental.pallas import tpu as pltpu
from jax.sharding import PartitionSpec as P

F32 = jnp.float32
BF16 = jnp.bfloat16
MESH = pl.DeviceIdType.MESH
LANES = 128
TILE = 512
RING = 4


def pick_target(logits, targets, column_start):
    column_ids = column_start + lax.broadcasted_iota(jnp.int32, logits.shape, 1)
    return jnp.sum(jnp.where(column_ids == targets[:, None], logits, 0.0), axis=1)


def stats_all(logits, targets, column_start):
    picked = pick_target(logits, targets, column_start)
    row_top = lax.pmax(jnp.max(logits, axis=1), ("grid", "rep"))
    local_total = jnp.sum(jnp.exp(logits - row_top[:, None]), axis=1)
    row_total, target_logit = lax.psum((local_total, picked), ("grid", "rep"))
    return target_logit - row_top - jnp.log(row_total)


def general(tokens, target_tokens, gate_weight, up_weight, down_weight, norm_gain, vocab_weight):
    own_rows = tokens.shape[0]
    width = tokens.shape[1] * lax.axis_size("row")
    copy_rows = lax.all_gather(tokens, "grid", axis=0, tiled=True)
    gate_part = jnp.dot(
        copy_rows,
        lax.all_gather(gate_weight, "rep", axis=0, tiled=True),
        preferred_element_type=F32,
    )
    up_part = jnp.dot(
        copy_rows,
        lax.all_gather(up_weight, "rep", axis=0, tiled=True),
        preferred_element_type=F32,
    )
    gate_value, up_value = lax.psum((gate_part, up_part), "row")
    hidden = (jax.nn.silu(gate_value) * up_value).astype(BF16)
    down_full = lax.all_gather(down_weight, "rep", axis=1, tiled=True)
    branch_sum = lax.psum_scatter(
        jnp.dot(hidden, down_full, preferred_element_type=F32),
        "grid",
        scatter_dimension=0,
        tiled=True,
    )
    mixed = (tokens.astype(F32) + branch_sum).astype(BF16)
    held = lax.optimization_barrier(mixed).astype(F32)
    squares = lax.psum(jnp.sum(held * held, axis=1), "row")
    scale = lax.rsqrt(squares / width + 1e-05)
    normed = (held * scale[:, None] * norm_gain[None, :]).astype(BF16)
    partial_logits = jnp.dot(
        lax.all_gather(normed, ("grid", "rep"), axis=0, tiled=True),
        vocab_weight,
        preferred_element_type=F32,
    )
    logits = lax.psum(partial_logits, "row")
    block_index = lax.axis_index(("grid", "rep"))
    column_start = block_index * vocab_weight.shape[1]
    every_logprob = stats_all(logits, target_tokens, column_start)
    logprob = lax.dynamic_slice_in_dim(every_logprob, block_index * own_rows, own_rows, 0)
    return (mixed, logprob)


def tiles(width):
    full = width // TILE
    return full, width - full * TILE


def over_tiles(width, step):
    full, rest = tiles(width)

    def one(n, carry):
        step(pl.ds(pl.multiple_of(n * TILE, TILE), TILE))
        return carry

    if full:
        lax.fori_loop(0, full, one, 0)
    if rest:
        step(pl.ds(full * TILE, rest))


class Sems:
    def __init__(self, send, recv):
        self.send, self.recv, self.used = send, recv, 0

    def take(self, count=1):
        first = self.used
        self.used += count
        return first


def block_kernel(
    tok_hbm, tgt_ref, gain_ref, wg_hbm, wu_hbm, wd_hbm, wv_hbm, mixed_hbm, lp_ref,
    WG, WU, WD, WV, TOKS, X, GU, RB, PS, PR, H, RSS, RSR, OWN, MX, NB, SQS, SQR, L, LR,
    TT, SA, ST, SR, send_sem, recv_sem, local_sem,
):
    z = lax.axis_index("grid")
    r = lax.axis_index("row")
    p = lax.axis_index("rep")
    own_rows = tok_hbm.shape[0]
    wave_rows = own_rows // 2
    chunk = wave_rows * 2
    quarter = chunk // 4
    dc = wg_hbm.shape[0]
    ff = wg_hbm.shape[1]
    vocab = wv_hbm.shape[1]
    width = 4 * dc

    row_peer = {"grid": z, "row": 1 - r, "rep": p}
    x_peer = {"grid": z, "row": r, "rep": 1 - p}

    def up(s):
        return lax.rem(z + s, RING)

    def down(s):
        return lax.rem(z + RING - s, RING)

    sems = Sems(send_sem, recv_sem)

    def remote(src, dst, sem, device):
        return pltpu.make_async_remote_copy(
            src_ref=src, dst_ref=dst, send_sem=send_sem.at[sem], recv_sem=recv_sem.at[sem],
            device_id=device, device_id_type=MESH,
        )

    open_sends = {}

    def send(src, dst, sem, device):
        copy = remote(src, dst, sem, device)
        copy.start()
        open_sends[sem] = copy

    def sent(sem):
        open_sends.pop(sem).wait_send()

    def arrived(dst, sem):
        remote(dst, dst, sem, row_peer).wait_recv()

    loads = []

    def load(src, dst, n):
        copy = pltpu.make_async_copy(src, dst, local_sem.at[n])
        copy.start()
        loads.append(copy)
        return copy

    tok_loads = []
    for w in range(2):
        rows = pl.ds(w * wave_rows, wave_rows)
        theirs = pl.ds(pl.multiple_of((1 - p) * dc, dc), dc)
        mine = pl.ds(pl.multiple_of(p * dc, dc), dc)
        tok_loads.append((
            load(tok_hbm.at[rows, theirs], TOKS.at[w], 2 * w),
            load(tok_hbm.at[rows, mine], X.at[z, w, p], 2 * w + 1),
        ))
    wg_load = load(wg_hbm, WG, 4)
    wu_load = load(wu_hbm, WU, 5)
    wd_load = load(wd_hbm, WD, 6)
    wv_load = load(wv_hbm, WV, 7)

    barrier = pltpu.get_barrier_semaphore()
    for s in range(RING):
        for dr in range(2):
            for dp in range(2):
                if s or dr or dp:
                    pl.semaphore_signal(
                        barrier, inc=1,
                        device_id={"grid": up(s), "row": lax.rem(r + dr, 2), "rep": lax.rem(p + dp, 2)},
                        device_id_type=MESH,
                    )
    pl.semaphore_wait(barrier, 4 * RING - 1)

    tok_x = [sems.take() for _ in range(2)]
    tok_z = [[None] + [sems.take() for _ in range(1, RING)] for _ in range(2)]
    for w in range(2):
        tok_loads[w][0].wait()
        send(TOKS.at[w], X.at[z, w, p], tok_x[w], x_peer)

    def spread_tokens(w):
        tok_loads[w][1].wait()
        arrived(X.at[z, w, 1 - p], tok_x[w])
        for s in range(1, RING):
            send(X.at[z, w], X.at[z, w], tok_z[w][s], {"grid": down(s), "row": r, "rep": p})

    n_chunks = 2 * RING
    order = [(0, s) for s in range(RING)] + [(1, s) for s in (1, 2, 3, 0)]
    dd = [sems.take() for _ in range(n_chunks)]
    xp = [sems.take() for _ in range(n_chunks)]
    xh = [sems.take() for _ in range(n_chunks)]
    dh = [sems.take() for _ in range(n_chunks)]
    df = [sems.take() for _ in range(n_chunks)]
    rs = [[None] + [sems.take() for _ in range(1, RING)] for _ in range(2)]

    def gate_up(c):
        w, s = order[c]
        zo = up(s)
        slot = c % 2
        if s:
            arrived(X.at[zo, w], tok_z[w][s])
        if c >= 2:
            sent(dd[c - 2])

        def step(cols):
            x = X[zo, w].reshape(chunk, dc)
            for g, weight in enumerate((WG, WU)):
                part = jnp.dot(x, weight[:, cols], preferred_element_type=F32)
                for a in range(2):
                    for b in range(2):
                        at = (2 * a + b) * quarter
                        GU[slot, a, b, g, :, cols] = part[at : at + quarter]

        over_tiles(ff, step)
        send(GU.at[slot, 1 - r], RB.at[slot], dd[c], row_peer)

    def sum_rows(c):
        slot = c % 2
        arrived(RB.at[slot], dd[c])
        if c >= 2:
            sent(xp[c - 2])
        if c >= 4:
            sent(df[c - 4])

        def step(cols):
            for g in range(2):
                PS[slot, g, :, cols] = (
                    GU[slot, r, 1 - p, g, :, cols] + RB[slot, 1 - p, g, :, cols]
                ).astype(BF16)
                GU[slot, r, p, g, :, cols] = GU[slot, r, p, g, :, cols] + RB[slot, p, g, :, cols]

        over_tiles(ff, step)
        send(PS.at[slot], PR.at[c % 4], xp[c], x_peer)

    def activate(c):
        slot = c % 2
        hs = c % 4
        arrived(PR.at[hs], xp[c])
        if c >= 4:
            sent(xh[c - 4])
            sent(dh[c - 4])

        def step(cols):
            gate = GU[slot, r, p, 0, :, cols] + PR[hs, 0, :, cols].astype(F32)
            up_value = GU[slot, r, p, 1, :, cols] + PR[hs, 1, :, cols].astype(F32)
            hidden = gate / (1.0 + jnp.exp(-gate)) * up_value
            H[hs, r, p, :, cols] = hidden.astype(BF16)

        over_tiles(ff, step)
        send(H.at[hs, r, p], H.at[hs, r, p], xh[c], x_peer)
        send(H.at[hs, r, p], H.at[hs, r, p], dh[c], row_peer)

    def pass_on(c):
        hs = c % 4
        arrived(H.at[hs, r, 1 - p], xh[c])
        send(H.at[hs, r, 1 - p], H.at[hs, r, 1 - p], df[c], row_peer)

    def project(c):
        w, s = order[c]
        hs = c % 4
        arrived(H.at[hs, 1 - r, p], dh[c])
        arrived(H.at[hs, 1 - r, 1 - p], df[c])

        def step(cols):
            h = H[hs].reshape(chunk, ff)
            part = jnp.dot(h, WD[:, cols], preferred_element_type=F32)
            if s:
                RSS[w, s - 1, :, cols] = part.astype(BF16)
            else:
                OWN[w, :, cols] = part

        over_tiles(dc, step)
        if s:
            send(RSS.at[w, s - 1], RSR.at[w, s - 1], rs[w][s], {"grid": up(s), "row": r, "rep": p})

    def finish_rows(w):
        for s in range(1, RING):
            arrived(RSR.at[w, s - 1], rs[w][s])

        def step(cols):
            total = OWN[w, :, cols]
            for s in range(1, RING):
                total = total + RSR[w, s - 1, :, cols].astype(F32)
            own = X[z, w, :, :, cols].reshape(chunk, cols.size).astype(F32)
            MX[z, w, p, :, cols] = (own + total).astype(BF16)

        over_tiles(dc, step)

    gx = [sems.take() for _ in range(2)]
    g0 = [None] + [sems.take() for _ in range(1, RING)]
    g1 = [None] + [sems.take() for _ in range(1, RING)]
    gf = [None] + [sems.take() for _ in range(1, RING)]

    def gather_first_x():
        send(MX.at[z, 0, p], MX.at[z, 0, p], gx[0], x_peer)

    def gather_first_z():
        arrived(MX.at[z, 0, 1 - p], gx[0])
        for s in (1, 3, 2):
            send(MX.at[z, 0], MX.at[z, 0], g0[s], {"grid": up(s), "row": r, "rep": p})

    def gather_last():
        for s in (1, 3, 2):
            send(MX.at[z, 1, p], MX.at[z, 1, p], g1[s], {"grid": up(s), "row": r, "rep": p})
        send(MX.at[z, 1, p], MX.at[z, 1, p], gx[1], x_peer)

    def forward_last(s):
        block = MX.at[down(s), 1, p]
        arrived(block, g1[s])
        send(block, block, gf[s], x_peer)

    spread_tokens(0)
    wg_load.wait()
    wu_load.wait()
    gate_up(0)
    spread_tokens(1)
    sum_rows(0)
    gate_up(1)
    sum_rows(1)
    for i in range(n_chunks + 1):
        if i < n_chunks:
            activate(i)
        if i + 2 < n_chunks:
            gate_up(i + 2)
        if i >= 1:
            pass_on(i - 1)
        if i + 2 < n_chunks:
            sum_rows(i + 2)
        if i == 1:
            wd_load.wait()
        if i >= 1:
            project(i - 1)
        if i == 5:
            finish_rows(0)
            gather_first_x()
        if i == 6:
            gather_first_z()
    finish_rows(1)
    gather_last()

    sq = [sems.take() for _ in range(n_chunks)]
    lg = [sems.take() for _ in range(n_chunks)]

    def squares(k, zb, w):
        def half(h):
            v = MX[zb, w, h].astype(F32)
            return jnp.sum(v * v, axis=1, keepdims=True)

        SQS[k] = jnp.broadcast_to(half(0) + half(1), (chunk, LANES))
        send(SQS.at[k], SQR.at[k], sq[k], row_peer)

    def normalise(k, zb, w):
        arrived(SQR.at[k], sq[k])
        scale = lax.rsqrt((SQS[k] + SQR[k])[:, :1] / width + 1e-05)
        for h in range(2):
            cols = slice(h * dc, (h + 1) * dc)
            v = MX[zb, w, h].astype(F32) * scale * gain_ref[:, cols]
            NB[k % RING, :, cols] = v.astype(BF16)

    def logits(k0, count, cols):
        x = NB[k0 % RING : k0 % RING + count].reshape(count * chunk, 2 * dc)
        part = jnp.dot(x, WV[:, cols], preferred_element_type=F32)
        for k in range(count):
            for a in range(2):
                at = k * chunk + a * wave_rows
                L[k0 % RING + k, a, :, cols] = part[at : at + wave_rows]

    def exchange(k0, count):
        for k in range(k0, k0 + count):
            send(L.at[k % RING, 1 - r], LR.at[k], lg[k], row_peer)

    column_start = ((z * 2 + p) * vocab).astype(F32)

    def stats(k, zb, w):
        arrived(LR.at[k], lg[k])
        full, rest = tiles(vocab)
        spans = [slice(n * TILE, (n + 1) * TILE) for n in range(full)]
        if rest:
            spans.append(slice(full * TILE, vocab))
        top = None
        for cols in spans:
            t = L[k % RING, r, :, cols] + LR[k, :, cols]
            L[k % RING, r, :, cols] = t
            m = jnp.max(t, axis=1, keepdims=True)
            top = m if top is None else jnp.maximum(top, m)
        rows = pl.ds(pl.multiple_of(r * own_rows + w * wave_rows, wave_rows), wave_rows)
        target = TT[zb, rows, :1] - column_start
        total = jnp.zeros((wave_rows, 1), F32)
        picked = jnp.zeros((wave_rows, 1), F32)
        for cols in spans:
            t = L[k % RING, r, :, cols]
            ids = (lax.broadcasted_iota(jnp.int32, t.shape, 1) + cols.start).astype(F32)
            total = total + jnp.sum(jnp.exp(t - top), axis=1, keepdims=True)
            picked = picked + jnp.sum(jnp.where(ids == target, t, 0.0), axis=1, keepdims=True)
        lane = lax.broadcasted_iota(jnp.int32, (wave_rows, LANES), 1)
        packed = jnp.where(lane == 0, top, jnp.where(lane == 1, total, picked))
        SA[zb, w * wave_rows : (w + 1) * wave_rows] = packed

    SA[...] = jnp.zeros_like(SA)
    for zb in range(RING):
        line = tgt_ref[zb].astype(F32)
        TT[zb] = jnp.broadcast_to(line, (LANES, LANES)).T

    first = [(zb, up(s)) for zb, s in enumerate((0, 1, 2, 3))]
    for s in (1, 3, 2):
        arrived(MX.at[down(s), 0], g0[s])
    for k, zb in first:
        squares(k, zb, 0)
    wv_load.wait()
    for k, zb in first:
        normalise(k, zb, 0)

    full, rest = tiles(vocab)
    marks = [0, (full + 2) // 3, (2 * full + 2) // 3, full]

    def logits_part(k0, count, start, stop):
        def one(n, carry):
            logits(k0, count, pl.ds(pl.multiple_of(n * TILE, TILE), TILE))
            return carry

        if stop > start:
            lax.fori_loop(start, stop, one, 0)

    logits_part(0, RING, marks[0], marks[1])
    forward_last(1)
    logits_part(0, RING, marks[1], marks[2])
    forward_last(3)
    logits_part(0, RING, marks[2], marks[3])
    if rest:
        logits(0, RING, pl.ds(full * TILE, rest))
    exchange(0, RING)

    second = [(4, z), (5, down(1)), (6, down(3)), (7, down(2))]
    arrived(MX.at[z, 1, 1 - p], gx[1])
    squares(4, z, 1)
    arrived(MX.at[down(1), 1, 1 - p], gf[1])
    squares(5, down(1), 1)
    forward_last(2)
    for k, zb in first:
        stats(k, zb, 0)
    for k in range(RING):
        sent(lg[k])
    for k, zb in second[:2]:
        normalise(k, zb, 1)
    over_tiles(vocab, lambda cols: logits(4, 2, cols))
    exchange(4, 2)
    arrived(MX.at[down(3), 1, 1 - p], gf[3])
    squares(6, down(3), 1)
    arrived(MX.at[down(2), 1, 1 - p], gf[2])
    squares(7, down(2), 1)

    outs = []
    for w in range(2):
        for h in range(2):
            rows = pl.ds(pl.multiple_of(p * wave_rows, wave_rows), wave_rows)
            copy = pltpu.make_async_copy(
                MX.at[z, w, h, rows],
                mixed_hbm.at[pl.ds(w * wave_rows, wave_rows), pl.ds(h * dc, dc)],
                local_sem.at[2 * w + h],
            )
            copy.start()
            outs.append(copy)

    for k, zb in second[2:]:
        normalise(k, zb, 1)
    over_tiles(vocab, lambda cols: logits(6, 2, cols))
    exchange(6, 2)
    for k, zb in second:
        stats(k, zb, 1)

    st = sems.take(2 * RING)
    base = sems.take(2 * RING)
    me = z * 2 + p
    for s in range(RING):
        ST[s] = SA[up(s)].T[:8]

    def figures(s, dr):
        device = {"grid": up(s), "row": lax.rem(r + dr, 2), "rep": r}
        return pltpu.make_async_remote_copy(
            src_ref=ST.at[s], dst_ref=SR.at[me],
            send_sem=send_sem.at[st + 2 * s + dr], recv_sem=recv_sem.at[base + me],
            device_id=device, device_id_type=MESH,
        )

    for s in (1, 2, 3, 0):
        for dr in range(2):
            if s or dr:
                figures(s, dr).start()

    @pl.when(p != r)
    def _():
        figures(0, 0).start()

    @pl.when(p == r)
    def _():
        SR[me] = ST[0]

    for s in range(RING):
        for dp in range(2):
            other = up(s) * 2 + lax.rem(p + dp, 2)
            wait = pltpu.make_async_remote_copy(
                src_ref=SR.at[other], dst_ref=SR.at[other],
                send_sem=send_sem.at[st], recv_sem=recv_sem.at[base + other],
                device_id=row_peer, device_id_type=MESH,
            )
            if s or dp:
                wait.wait_recv()
            else:
                @pl.when(p != r)
                def _():
                    wait.wait_recv()

    top = SR[0, 0:1]
    for n in range(1, 2 * RING):
        top = jnp.maximum(top, SR[n, 0:1])
    total = jnp.zeros_like(top)
    picked = jnp.zeros_like(top)
    for n in range(2 * RING):
        total = total + SR[n, 1:2] * jnp.exp(SR[n, 0:1] - top)
        picked = picked + SR[n, 2:3]
    lp_ref[...] = picked - top - jnp.log(total)

    for s in range(RING):
        for dr in range(2):
            if s or dr:
                figures(s, dr).wait_send()

    @pl.when(p != r)
    def _():
        figures(0, 0).wait_send()

    for sem in list(open_sends):
        sent(sem)
    for copy in outs:
        copy.wait()


N_SEMS = 128


def block(tokens, target_tokens, gate_weight, up_weight, down_weight, norm_gain, vocab_weight):
    own_rows, half_width = tokens.shape
    wave_rows = own_rows // 2
    chunk = 2 * wave_rows
    quarter = chunk // 4
    dc, ff = gate_weight.shape
    vocab = vocab_weight.shape[1]
    vmem = pltpu.VMEM
    any_space = pl.BlockSpec(memory_space=pl.ANY)
    in_vmem = pl.BlockSpec(memory_space=pltpu.VMEM)
    targets = target_tokens.reshape(RING, 1, 2 * own_rows)
    gain = norm_gain.reshape(1, half_width)
    mixed, logprob = pl.pallas_call(
        block_kernel,
        out_shape=(
            jax.ShapeDtypeStruct((own_rows, half_width), BF16),
            jax.ShapeDtypeStruct((1, LANES), F32),
        ),
        in_specs=[any_space, in_vmem, in_vmem, any_space, any_space, any_space, any_space],
        out_specs=(any_space, in_vmem),
        scratch_shapes=[
            vmem((dc, ff), BF16),
            vmem((dc, ff), BF16),
            vmem((ff, dc), BF16),
            vmem((half_width, vocab), BF16),
            vmem((2, wave_rows, dc), BF16),
            vmem((RING, 2, 2, wave_rows, dc), BF16),
            vmem((2, 2, 2, 2, quarter, ff), F32),
            vmem((2, 2, 2, quarter, ff), F32),
            vmem((2, 2, quarter, ff), BF16),
            vmem((4, 2, quarter, ff), BF16),
            vmem((4, 2, 2, quarter, ff), BF16),
            vmem((2, RING - 1, chunk, dc), BF16),
            vmem((2, RING - 1, chunk, dc), BF16),
            vmem((2, chunk, dc), F32),
            vmem((RING, 2, 2, chunk, dc), BF16),
            vmem((RING, chunk, half_width), BF16),
            vmem((2 * RING, chunk, LANES), F32),
            vmem((2 * RING, chunk, LANES), F32),
            vmem((RING, 2, wave_rows, vocab), F32),
            vmem((2 * RING, wave_rows, vocab), F32),
            vmem((RING, LANES, LANES), F32),
            vmem((RING, LANES, LANES), F32),
            vmem((RING, 8, LANES), F32),
            vmem((2 * RING, 8, LANES), F32),
            pltpu.SemaphoreType.DMA((N_SEMS,)),
            pltpu.SemaphoreType.DMA((N_SEMS,)),
            pltpu.SemaphoreType.DMA((8,)),
        ],
        compiler_params=pltpu.CompilerParams(
            collective_id=0, has_side_effects=True, vmem_limit_bytes=67_043_328
        ),
        name="block",
    )(tokens, targets, gain, gate_weight, up_weight, down_weight, vocab_weight)
    return (mixed, logprob[0, :own_rows])


def solution(mesh):
    in_specs = (
        P(("groups", "grid", "rep"), "row"),
        P("groups"),
        P(("row", "rep"), "grid"),
        P(("row", "rep"), "grid"),
        P("grid", ("row", "rep")),
        P("row"),
        P("row", ("grid", "rep")),
    )
    out_specs = (P(("groups", "grid", "rep"), "row"), P(("groups", "grid", "rep")))
    small = mesh.shape["row"] == 2 and mesh.shape["rep"] == 2 and mesh.shape["grid"] == RING
    return jax.shard_map(
        block if small else general,
        mesh=mesh,
        in_specs=in_specs,
        out_specs=out_specs,
        check_vma=False,
    )
```

```python
import jax
import jax.numpy as jnp
from jax import lax
from jax.experimental import pallas as pl
from jax.experimental.pallas import tpu as pltpu
from jax.sharding import PartitionSpec as P

F32 = jnp.float32
BF16 = jnp.bfloat16
MESH = pl.DeviceIdType.MESH
LANES = 128
TILE = 512
GATE_TILE = 1792
PROJECT_TILE = 1024
RING = 4


def pick_target(logits, targets, column_start):
    column_ids = column_start + lax.broadcasted_iota(jnp.int32, logits.shape, 1)
    return jnp.sum(jnp.where(column_ids == targets[:, None], logits, 0.0), axis=1)


def stats_all(logits, targets, column_start):
    picked = pick_target(logits, targets, column_start)
    row_top = lax.pmax(jnp.max(logits, axis=1), ("grid", "rep"))
    local_total = jnp.sum(jnp.exp(logits - row_top[:, None]), axis=1)
    row_total, target_logit = lax.psum((local_total, picked), ("grid", "rep"))
    return target_logit - row_top - jnp.log(row_total)


def general(tokens, target_tokens, gate_weight, up_weight, down_weight, norm_gain, vocab_weight):
    own_rows = tokens.shape[0]
    width = tokens.shape[1] * lax.axis_size("row")
    copy_rows = lax.all_gather(tokens, "grid", axis=0, tiled=True)
    gate_part = jnp.dot(
        copy_rows,
        lax.all_gather(gate_weight, "rep", axis=0, tiled=True),
        preferred_element_type=F32,
    )
    up_part = jnp.dot(
        copy_rows,
        lax.all_gather(up_weight, "rep", axis=0, tiled=True),
        preferred_element_type=F32,
    )
    gate_value, up_value = lax.psum((gate_part, up_part), "row")
    hidden = (jax.nn.silu(gate_value) * up_value).astype(BF16)
    down_full = lax.all_gather(down_weight, "rep", axis=1, tiled=True)
    branch_sum = lax.psum_scatter(
        jnp.dot(hidden, down_full, preferred_element_type=F32),
        "grid",
        scatter_dimension=0,
        tiled=True,
    )
    mixed = (tokens.astype(F32) + branch_sum).astype(BF16)
    held = lax.optimization_barrier(mixed).astype(F32)
    squares = lax.psum(jnp.sum(held * held, axis=1), "row")
    scale = lax.rsqrt(squares / width + 1e-05)
    normed = (held * scale[:, None] * norm_gain[None, :]).astype(BF16)
    partial_logits = jnp.dot(
        lax.all_gather(normed, ("grid", "rep"), axis=0, tiled=True),
        vocab_weight,
        preferred_element_type=F32,
    )
    logits = lax.psum(partial_logits, "row")
    block_index = lax.axis_index(("grid", "rep"))
    column_start = block_index * vocab_weight.shape[1]
    every_logprob = stats_all(logits, target_tokens, column_start)
    logprob = lax.dynamic_slice_in_dim(every_logprob, block_index * own_rows, own_rows, 0)
    return (mixed, logprob)


def tiles(width, tile=TILE):
    full = width // tile
    return full, width - full * tile


def over_tiles(width, step, tile=TILE):
    full, rest = tiles(width, tile)

    def one(n, carry):
        step(pl.ds(pl.multiple_of(n * tile, tile), tile))
        return carry

    if full == 1:
        step(pl.ds(0, tile))
    elif full:
        lax.fori_loop(0, full, one, 0)
    if rest:
        step(pl.ds(full * tile, rest))


class Sems:
    def __init__(self, send, recv):
        self.send, self.recv, self.used = send, recv, 0

    def take(self, count=1):
        first = self.used
        self.used += count
        return first


def block_kernel(
    tok_hbm, tgt_ref, gain_ref, wg_hbm, wu_hbm, wd_hbm, wv_hbm, mixed_hbm, lp_ref,
    WG, WU, WD, WV, TOKS, X, GU, RB, PS, PR, H, RSS, RSR, OWN, MX, NB, SQS, SQR, L, LR,
    TG, ST, SR, send_sem, recv_sem, local_sem,
):
    z = lax.axis_index("grid")
    r = lax.axis_index("row")
    p = lax.axis_index("rep")
    own_rows = tok_hbm.shape[0]
    wave_rows = own_rows // 2
    chunk = wave_rows * 2
    quarter = chunk // 4
    dc = wg_hbm.shape[0]
    ff = wg_hbm.shape[1]
    vocab = wv_hbm.shape[0]
    width = 4 * dc

    row_peer = {"grid": z, "row": 1 - r, "rep": p}
    x_peer = {"grid": z, "row": r, "rep": 1 - p}

    def pal(s):
        return (z, z + 1 - 2 * lax.rem(z, 2), lax.rem(z + 2, RING), RING - 1 - z)[s]

    def at_grid(there):
        return {"grid": there, "row": r, "rep": p}

    sems = Sems(send_sem, recv_sem)

    def remote(src, dst, sem, device):
        return pltpu.make_async_remote_copy(
            src_ref=src, dst_ref=dst, send_sem=send_sem.at[sem], recv_sem=recv_sem.at[sem],
            device_id=device, device_id_type=MESH,
        )

    open_sends = {}

    def send(src, dst, sem, device):
        copy = remote(src, dst, sem, device)
        copy.start()
        open_sends[sem] = copy

    def sent(sem):
        open_sends.pop(sem).wait_send()

    def arrived(dst, sem):
        remote(dst, dst, sem, row_peer).wait_recv()

    loads = []

    def load(src, dst, n):
        copy = pltpu.make_async_copy(src, dst, local_sem.at[n])
        copy.start()
        loads.append(copy)
        return copy

    tok_loads = []
    for w in range(2):
        rows = pl.ds(w * wave_rows, wave_rows)
        theirs = pl.ds(pl.multiple_of((1 - p) * dc, dc), dc)
        mine = pl.ds(pl.multiple_of(p * dc, dc), dc)
        tok_loads.append((
            load(tok_hbm.at[rows, theirs], TOKS.at[w], 2 * w),
            load(tok_hbm.at[rows, mine], X.at[z, w, p], 2 * w + 1),
        ))
    wg_load = load(wg_hbm, WG, 4)
    wu_load = load(wu_hbm, WU, 5)
    wd_load = load(wd_hbm, WD, 6)
    wv_load = load(wv_hbm, WV, 7)

    barrier = pltpu.get_barrier_semaphore()
    for s in range(RING):
        for dr in range(2):
            for dp in range(2):
                if s or dr or dp:
                    pl.semaphore_signal(
                        barrier, inc=1,
                        device_id={"grid": lax.rem(z + s, RING), "row": lax.rem(r + dr, 2), "rep": lax.rem(p + dp, 2)},
                        device_id_type=MESH,
                    )
    pl.semaphore_wait(barrier, 4 * RING - 1)

    tok_x = [sems.take() for _ in range(2)]
    near = [sems.take() for _ in range(2)]
    tok_z = [[None] + [sems.take() for _ in range(1, RING)] for _ in range(2)]
    tok_loads[0][0].wait()
    send(TOKS.at[0], X.at[z, 0, p], tok_x[0], x_peer)
    tok_loads[0][1].wait()
    send(X.at[z, 0, p], X.at[z, 0, p], near[0], at_grid(pal(1)))
    send(TOKS.at[0], X.at[z, 0, p], near[1], {"grid": pal(1), "row": r, "rep": 1 - p})
    tok_loads[1][0].wait()
    send(TOKS.at[1], X.at[z, 1, p], tok_x[1], x_peer)
    tok_loads[1][1].wait()

    def take_tokens(w):
        arrived(X.at[z, w, 1 - p], tok_x[w])

    def spread_tokens(w, distances):
        for s in distances:
            send(X.at[z, w], X.at[z, w], tok_z[w][s], at_grid(pal(s)))

    n_chunks = 2 * RING
    order = [(0, s) for s in range(RING)] + [(1, s) for s in (1, 2, 3, 0)]
    dd = [[sems.take() for _ in range(2)] for _ in range(n_chunks)]
    xp = [sems.take() for _ in range(n_chunks)]
    xh = [sems.take() for _ in range(n_chunks)]
    dh = [sems.take() for _ in range(n_chunks)]
    df = [sems.take() for _ in range(n_chunks)]
    rs = [[None] + [sems.take() for _ in range(1, RING)] for _ in range(2)]

    def gate_up(c):
        w, s = order[c]
        zo = pal(s)
        slot = c % 2
        if s == 1 and w == 0:
            arrived(X.at[zo, w, p], near[0])
            arrived(X.at[zo, w, 1 - p], near[1])
        elif s:
            arrived(X.at[zo, w], tok_z[w][s])
        for g, weight in enumerate((WG, WU)):
            if c >= 2:
                sent(dd[c - 2][g])

            def step(cols):
                x = X[zo, w].reshape(chunk, dc)
                part = jnp.dot(x, weight[:, cols], preferred_element_type=F32)
                for a in range(2):
                    for b in range(2):
                        at = (2 * a + b) * quarter
                        GU[slot, a, g, b, :, cols] = part[at : at + quarter]

            over_tiles(ff, step, GATE_TILE)
            send(GU.at[slot, 1 - r, g], RB.at[slot, g], dd[c][g], row_peer)

    def sum_rows(c):
        slot = c % 2
        if c >= 2:
            sent(xp[c - 2])
        if c >= 4:
            sent(df[c - 4])
        for g in range(2):
            arrived(RB.at[slot, g], dd[c][g])

            def step(cols):
                PS[slot, g, :, cols] = (
                    GU[slot, r, g, 1 - p, :, cols] + RB[slot, g, 1 - p, :, cols]
                ).astype(BF16)
                GU[slot, r, g, p, :, cols] = GU[slot, r, g, p, :, cols] + RB[slot, g, p, :, cols]

            over_tiles(ff, step)
        send(PS.at[slot], PR.at[c % 4], xp[c], x_peer)

    def activate(c):
        slot = c % 2
        hs = c % 4
        arrived(PR.at[hs], xp[c])
        if c >= 4:
            sent(xh[c - 4])
            sent(dh[c - 4])

        def step(cols):
            gate = GU[slot, r, 0, p, :, cols] + PR[hs, 0, :, cols].astype(F32)
            up_value = GU[slot, r, 1, p, :, cols] + PR[hs, 1, :, cols].astype(F32)
            hidden = gate / (1.0 + jnp.exp(-gate)) * up_value
            H[hs, r, p, :, cols] = hidden.astype(BF16)

        over_tiles(ff, step)
        send(H.at[hs, r, p], H.at[hs, r, p], xh[c], x_peer)
        send(H.at[hs, r, p], H.at[hs, r, p], dh[c], row_peer)

    def pass_on(c):
        hs = c % 4
        arrived(H.at[hs, r, 1 - p], xh[c])
        send(H.at[hs, r, 1 - p], H.at[hs, r, 1 - p], df[c], row_peer)

    def project(c):
        w, s = order[c]
        hs = c % 4
        arrived(H.at[hs, 1 - r, p], dh[c])
        arrived(H.at[hs, 1 - r, 1 - p], df[c])

        def step(cols):
            h = H[hs].reshape(chunk, ff)
            part = jnp.dot(h, WD[:, cols], preferred_element_type=F32)
            if s:
                RSS[w, s - 1, :, cols] = part.astype(BF16)
            else:
                OWN[w, :, cols] = part

        over_tiles(dc, step, PROJECT_TILE)
        if s:
            send(RSS.at[w, s - 1], RSR.at[w, s - 1], rs[w][s], at_grid(pal(s)))

    def finish_rows(w):
        for s in range(1, RING):
            arrived(RSR.at[w, s - 1], rs[w][s])

        def step(cols):
            total = OWN[w, :, cols]
            for s in range(1, RING):
                total = total + RSR[w, s - 1, :, cols].astype(F32)
            own = X[z, w, :, :, cols].reshape(chunk, cols.size).astype(F32)
            MX[z, w, p, :, cols] = (own + total).astype(BF16)

        over_tiles(dc, step)

    gx = [sems.take() for _ in range(2)]
    hn = [sems.take() for _ in range(2)]
    hi = [sems.take(2) for _ in range(2)]
    ho = [[sems.take() for _ in range(2)] for _ in range(2)]
    g1 = [None] + [sems.take() for _ in range(1, RING)]
    gf = [None] + [sems.take() for _ in range(1, RING)]
    at_end = jnp.logical_or(z == 0, z == RING - 1)
    inside = jnp.logical_and(z > 0, z < RING - 1)
    inner = jnp.where(z < RING // 2, RING // 2, RING // 2 - 1)
    end_bit = 1 - jnp.where(inside, 1, 0)

    def gather_first_x():
        send(MX.at[z, 0, p], MX.at[z, 0, p], gx[0], x_peer)

    def part_of(h):
        return p if h == 0 else 1 - p

    def to_inner(h):
        block = MX.at[z, 0, part_of(h)]
        return pltpu.make_async_remote_copy(
            src_ref=block, dst_ref=block,
            send_sem=send_sem.at[hi[h]], recv_sem=recv_sem.at[hi[h] + end_bit],
            device_id=at_grid(inner), device_id_type=MESH,
        )

    def gather_first_z(h):
        block = MX.at[z, 0, part_of(h)]
        to_inner(h).start()
        send(block, block, hn[h], at_grid(pal(1)))

    def outward(h, j):
        block = MX.at[pal(3 - j), 0, part_of(h)]
        return remote(block, block, ho[h][j], at_grid(pal(1)))

    def hand_on(h):
        @pl.when(inside)
        def _():
            for j in range(2):
                arrived(MX.at[pal(3 - j), 0, part_of(h)], hi[h] + j)
                outward(h, j).start()

    def end_first(h):
        arrived(MX.at[pal(1), 0, part_of(h)], hn[h])

        @pl.when(at_end)
        def _():
            for j in range(2):
                arrived(MX.at[pal(2 + j), 0, part_of(h)], ho[h][j])

    def drain_first(h):
        to_inner(h).wait_send()

        @pl.when(inside)
        def _():
            for j in range(2):
                outward(h, j).wait_send()

    def gather_last():
        for s in (1, 2, 3):
            send(MX.at[z, 1, p], MX.at[z, 1, p], g1[s], at_grid(pal(s)))
        send(MX.at[z, 1, p], MX.at[z, 1, p], gx[1], x_peer)

    def forward_last(s):
        block = MX.at[pal(s), 1, p]
        arrived(block, g1[s])
        send(block, block, gf[s], x_peer)

    take_tokens(0)
    spread_tokens(0, (2, 3))
    wg_load.wait()
    wu_load.wait()
    gate_up(0)
    sum_rows(0)
    gate_up(1)
    sum_rows(1)
    take_tokens(1)
    spread_tokens(1, (1,))
    for i in range(n_chunks + 1):
        if i < n_chunks:
            activate(i)
        if i + 2 < n_chunks:
            gate_up(i + 2)
        if i >= 1:
            pass_on(i - 1)
        if i == 5:
            finish_rows(0)
            gather_first_x()
            gather_first_z(0)
        if i + 2 < n_chunks:
            sum_rows(i + 2)
        if i == 1:
            wd_load.wait()
            spread_tokens(1, (2, 3))
        if i >= 1:
            project(i - 1)
        if i == 6:
            arrived(MX.at[z, 0, 1 - p], gx[0])
            gather_first_z(1)
            hand_on(0)
        if i == 7:
            hand_on(1)
    finish_rows(1)
    gather_last()

    sq = [sems.take() for _ in range(n_chunks)]
    lg = [[sems.take() for _ in range(2)] for _ in range(2)]
    half = vocab // 2
    rows_tile = max(t for t in range(16, TILE + 1, 16) if half % t == 0)
    here = lax.div(z, 2)
    there = 1 - here

    def squares(k, zb, w):
        def part(h):
            v = MX[zb, w, h].astype(F32)
            return jnp.sum(v * v, axis=1, keepdims=True)

        SQS[k] = jnp.broadcast_to(part(0) + part(1), (chunk, LANES))
        send(SQS.at[k], SQR.at[k], sq[k], row_peer)

    def normalise(k, zb, w):
        arrived(SQR.at[k], sq[k])
        scale = lax.rsqrt((SQS[k] + SQR[k])[:, :1] / width + 1e-05)
        for h in range(2):
            cols = slice(h * dc, (h + 1) * dc)
            v = MX[zb, w, h].astype(F32) * scale * gain_ref[:, cols]
            NB[lax.div(zb, 2), lax.rem(zb, 2), :, cols] = v.astype(BF16)

    def logits_half(side, group):
        def step(n, carry):
            at = pl.multiple_of(n * rows_tile, 16)
            rows = pl.ds(pl.multiple_of(side * half + at, 16), rows_tile)
            x = NB[...] if group is None else NB[group]
            x = x.reshape(-1, 2 * dc)
            part = lax.dot_general(
                WV[rows, :], x, (((1,), (1,)), ((), ())), preferred_element_type=F32
            )
            if group is None:
                for g in range(2):
                    L[g, side, pl.ds(at, rows_tile)] = part[:, g * LANES : (g + 1) * LANES]
            else:
                L[group, side, pl.ds(at, rows_tile)] = part
            return carry

        lax.fori_loop(0, half // rows_tile, step, 0)

    def exchange(w, n, group):
        send(L.at[group, 1 - r], LR.at[w, group], lg[w][n], row_peer)

    row_start = (z * 2 + p) * vocab + r * half

    def stats(w, n, group):
        arrived(LR.at[w, group], lg[w][n])
        step_rows = rows_tile
        steps = half // step_rows

        def add(i, top):
            rows = pl.ds(pl.multiple_of(i * step_rows, 8), step_rows)
            t = L[group, r, rows] + LR[w, group, rows]
            L[group, r, rows] = t
            return jnp.maximum(top, jnp.max(t.reshape(-1, 8, LANES), axis=0))

        top = lax.fori_loop(0, steps, add, jnp.full((8, LANES), -jnp.inf, F32))
        top = jnp.max(top, axis=0, keepdims=True)
        target = TG[w, group, 0:1] - row_start

        def count(i, carry):
            total, picked = carry
            rows = pl.ds(pl.multiple_of(i * step_rows, 8), step_rows)
            t = L[group, r, rows]
            ids = lax.broadcasted_iota(jnp.int32, t.shape, 0) + i * step_rows
            e = jnp.exp(t - top)
            hit = jnp.where(ids == target, t, 0.0)
            return (
                total + jnp.sum(e.reshape(-1, 8, LANES), axis=0),
                picked + jnp.sum(hit.reshape(-1, 8, LANES), axis=0),
            )

        zero = jnp.zeros((8, LANES), F32)
        total, picked = lax.fori_loop(0, steps, count, (zero, zero))
        ST[group, 4 * w : 4 * w + 1] = top
        ST[group, 4 * w + 1 : 4 * w + 2] = jnp.sum(total, axis=0, keepdims=True)
        ST[group, 4 * w + 2 : 4 * w + 3] = jnp.sum(picked, axis=0, keepdims=True)

    lane = lax.broadcasted_iota(jnp.int32, (8, LANES), 1)
    ST[...] = jnp.zeros_like(ST)
    for g in range(2):
        for w in range(2):
            line = None
            for spot in range(4):
                source = 2 * (spot % 2) + w
                ids = jnp.broadcast_to(tgt_ref[2 * g + spot // 2], (8, LANES))
                ids = pltpu.roll(ids, ((spot - source) * wave_rows) % LANES, 1)
                line = ids if line is None else jnp.where(lane >= spot * wave_rows, ids, line)
            TG[w, g] = line

    first = [(s, pal(s)) for s in range(RING)]
    end_first(0)
    end_first(1)
    for k, zb in first:
        squares(k, zb, 0)
    wv_load.wait()
    for k, zb in first:
        normalise(k, zb, 0)
    logits_half(1 - r, None)
    for g in range(2):
        exchange(0, g, g)
    forward_last(1)
    logits_half(r, None)
    forward_last(2)
    arrived(MX.at[z, 1, 1 - p], gx[1])
    squares(4, z, 1)
    arrived(MX.at[pal(1), 1, 1 - p], gf[1])
    squares(5, pal(1), 1)
    outs = []
    for w in range(2):
        for h in range(2):
            rows = pl.ds(pl.multiple_of(p * wave_rows, wave_rows), wave_rows)
            copy = pltpu.make_async_copy(
                MX.at[z, w, h, rows],
                mixed_hbm.at[pl.ds(w * wave_rows, wave_rows), pl.ds(h * dc, dc)],
                local_sem.at[2 * w + h],
            )
            copy.start()
            outs.append(copy)

    for g in range(2):
        stats(0, g, g)
    for g in range(2):
        sent(lg[0][g])
    normalise(4, z, 1)
    normalise(5, pal(1), 1)
    logits_half(1 - r, here)
    exchange(1, 0, here)
    forward_last(3)
    logits_half(r, here)
    for s in (2, 3):
        arrived(MX.at[pal(s), 1, 1 - p], gf[s])
        squares(RING + s, pal(s), 1)
    stats(1, 0, here)
    for s in (2, 3):
        normalise(RING + s, pal(s), 1)
    logits_half(1 - r, there)
    exchange(1, 1, there)
    logits_half(r, there)
    stats(1, 1, there)

    n_all = 4 * RING
    st = sems.take(n_all)
    base = sems.take(n_all)
    me = (z * 2 + r) * 2 + p

    def others():
        for s in (3, 2, 1, 0):
            for dr in range(2):
                for dp in range(2):
                    if s or dr or dp:
                        yield s, dr, dp

    def figures(s, dr, dp):
        device = {"grid": pal(s), "row": lax.rem(r + dr, 2), "rep": lax.rem(p + dp, 2)}
        return pltpu.make_async_remote_copy(
            src_ref=ST.at[lax.div(pal(s), 2)], dst_ref=SR.at[me],
            send_sem=send_sem.at[st + 4 * s + 2 * dr + dp], recv_sem=recv_sem.at[base + me],
            device_id=device, device_id_type=MESH,
        )

    for other in others():
        figures(*other).start()
    SR[me] = ST[here]
    for s, dr, dp in others():
        who = (pal(s) * 2 + lax.rem(r + dr, 2)) * 2 + lax.rem(p + dp, 2)
        arrived(SR.at[who], base + who)

    lines = []
    for w in range(2):
        top = SR[0, 4 * w : 4 * w + 1]
        for n in range(1, n_all):
            top = jnp.maximum(top, SR[n, 4 * w : 4 * w + 1])
        total = jnp.zeros_like(top)
        picked = jnp.zeros_like(top)
        for n in range(n_all):
            total = total + SR[n, 4 * w + 1 : 4 * w + 2] * jnp.exp(SR[n, 4 * w : 4 * w + 1] - top)
            picked = picked + SR[n, 4 * w + 2 : 4 * w + 3]
        lines.append(jnp.broadcast_to(picked - top - jnp.log(total), (8, LANES)))
    spot = lax.rem(z, 2) * 2 + p
    result = jnp.zeros((8, LANES), F32)
    for k in range(4):
        a = pltpu.roll(lines[0], (-k * wave_rows) % LANES, 1)
        b = pltpu.roll(lines[1], ((1 - k) * wave_rows) % LANES, 1)
        result = jnp.where(spot == k, jnp.where(lane < wave_rows, a, b), result)
    lp_ref[...] = result[0:1]

    for other in others():
        figures(*other).wait_send()
    for h in range(2):
        drain_first(h)
    for sem in list(open_sends):
        sent(sem)
    for copy in outs:
        copy.wait()


N_SEMS = 160


def block(tokens, target_tokens, gate_weight, up_weight, down_weight, norm_gain, vocab_weight):
    own_rows, half_width = tokens.shape
    wave_rows = own_rows // 2
    chunk = 2 * wave_rows
    quarter = chunk // 4
    dc, ff = gate_weight.shape
    vocab = vocab_weight.shape[1]
    vmem = pltpu.VMEM
    any_space = pl.BlockSpec(memory_space=pl.ANY)
    in_vmem = pl.BlockSpec(memory_space=pltpu.VMEM)
    targets = target_tokens.reshape(RING, 1, 2 * own_rows)
    gain = norm_gain.reshape(1, half_width)
    mixed, logprob = pl.pallas_call(
        block_kernel,
        out_shape=(
            jax.ShapeDtypeStruct((own_rows, half_width), BF16),
            jax.ShapeDtypeStruct((1, LANES), F32),
        ),
        in_specs=[any_space, in_vmem, in_vmem, any_space, any_space, any_space, any_space],
        out_specs=(any_space, in_vmem),
        scratch_shapes=[
            vmem((dc, ff), BF16),
            vmem((dc, ff), BF16),
            vmem((ff, dc), BF16),
            vmem((vocab, half_width), BF16),
            vmem((2, wave_rows, dc), BF16),
            vmem((RING, 2, 2, wave_rows, dc), BF16),
            vmem((2, 2, 2, 2, quarter, ff), F32),
            vmem((2, 2, 2, quarter, ff), F32),
            vmem((2, 2, quarter, ff), BF16),
            vmem((4, 2, quarter, ff), BF16),
            vmem((4, 2, 2, quarter, ff), BF16),
            vmem((2, RING - 1, chunk, dc), BF16),
            vmem((2, RING - 1, chunk, dc), BF16),
            vmem((2, chunk, dc), F32),
            vmem((RING, 2, 2, chunk, dc), BF16),
            vmem((2, 2, chunk, half_width), BF16),
            vmem((2 * RING, chunk, LANES), F32),
            vmem((2 * RING, chunk, LANES), F32),
            vmem((2, 2, vocab // 2, LANES), F32),
            vmem((2, 2, vocab // 2, LANES), F32),
            vmem((2, 2, 8, LANES), jnp.int32),
            vmem((2, 8, LANES), F32),
            vmem((4 * RING, 8, LANES), F32),
            pltpu.SemaphoreType.DMA((N_SEMS,)),
            pltpu.SemaphoreType.DMA((N_SEMS,)),
            pltpu.SemaphoreType.DMA((8,)),
        ],
        compiler_params=pltpu.CompilerParams(
            collective_id=0, has_side_effects=True, vmem_limit_bytes=67_043_328
        ),
        name="block",
    )(tokens, targets, gain, gate_weight, up_weight, down_weight, vocab_weight.T)
    return (mixed, logprob[0, :own_rows])


def solution(mesh):
    in_specs = (
        P(("groups", "grid", "rep"), "row"),
        P("groups"),
        P(("row", "rep"), "grid"),
        P(("row", "rep"), "grid"),
        P("grid", ("row", "rep")),
        P("row"),
        P("row", ("grid", "rep")),
    )
    out_specs = (P(("groups", "grid", "rep"), "row"), P(("groups", "grid", "rep")))
    small = mesh.shape["row"] == 2 and mesh.shape["rep"] == 2 and mesh.shape["grid"] == RING
    return jax.shard_map(
        block if small else general,
        mesh=mesh,
        in_specs=in_specs,
        out_specs=out_specs,
        check_vma=False,
    )
```

```python
import jax
import jax.numpy as jnp
from jax import lax
from jax.experimental import pallas as pl
from jax.experimental.pallas import tpu as pltpu
from jax.sharding import PartitionSpec as P

F32 = jnp.float32
BF16 = jnp.bfloat16
MESH = pl.DeviceIdType.MESH
LANES = 128
TILE = 512
GATE_TILE = 1792
PROJECT_TILE = 1024
RING = 4


def pick_target(logits, targets, column_start):
    column_ids = column_start + lax.broadcasted_iota(jnp.int32, logits.shape, 1)
    return jnp.sum(jnp.where(column_ids == targets[:, None], logits, 0.0), axis=1)


def stats_all(logits, targets, column_start):
    picked = pick_target(logits, targets, column_start)
    row_top = lax.pmax(jnp.max(logits, axis=1), ("grid", "rep"))
    local_total = jnp.sum(jnp.exp(logits - row_top[:, None]), axis=1)
    row_total, target_logit = lax.psum((local_total, picked), ("grid", "rep"))
    return target_logit - row_top - jnp.log(row_total)


def general(tokens, target_tokens, gate_weight, up_weight, down_weight, norm_gain, vocab_weight):
    own_rows = tokens.shape[0]
    width = tokens.shape[1] * lax.axis_size("row")
    copy_rows = lax.all_gather(tokens, "grid", axis=0, tiled=True)
    gate_part = jnp.dot(
        copy_rows,
        lax.all_gather(gate_weight, "rep", axis=0, tiled=True),
        preferred_element_type=F32,
    )
    up_part = jnp.dot(
        copy_rows,
        lax.all_gather(up_weight, "rep", axis=0, tiled=True),
        preferred_element_type=F32,
    )
    gate_value, up_value = lax.psum((gate_part, up_part), "row")
    hidden = (jax.nn.silu(gate_value) * up_value).astype(BF16)
    down_full = lax.all_gather(down_weight, "rep", axis=1, tiled=True)
    branch_sum = lax.psum_scatter(
        jnp.dot(hidden, down_full, preferred_element_type=F32),
        "grid",
        scatter_dimension=0,
        tiled=True,
    )
    mixed = (tokens.astype(F32) + branch_sum).astype(BF16)
    held = lax.optimization_barrier(mixed).astype(F32)
    squares = lax.psum(jnp.sum(held * held, axis=1), "row")
    scale = lax.rsqrt(squares / width + 1e-05)
    normed = (held * scale[:, None] * norm_gain[None, :]).astype(BF16)
    partial_logits = jnp.dot(
        lax.all_gather(normed, ("grid", "rep"), axis=0, tiled=True),
        vocab_weight,
        preferred_element_type=F32,
    )
    logits = lax.psum(partial_logits, "row")
    block_index = lax.axis_index(("grid", "rep"))
    column_start = block_index * vocab_weight.shape[1]
    every_logprob = stats_all(logits, target_tokens, column_start)
    logprob = lax.dynamic_slice_in_dim(every_logprob, block_index * own_rows, own_rows, 0)
    return (mixed, logprob)


def tiles(width, tile=TILE):
    full = width // tile
    return full, width - full * tile


def over_tiles(width, step, tile=TILE):
    full, rest = tiles(width, tile)

    def one(n, carry):
        step(pl.ds(pl.multiple_of(n * tile, tile), tile))
        return carry

    if full == 1:
        step(pl.ds(0, tile))
    elif full:
        lax.fori_loop(0, full, one, 0)
    if rest:
        step(pl.ds(full * tile, rest))


class Sems:
    def __init__(self, send, recv):
        self.send, self.recv, self.used = send, recv, 0

    def take(self, count=1):
        first = self.used
        self.used += count
        return first


def block_kernel(
    tok_hbm, tgt_ref, gain_ref, wg_hbm, wu_hbm, wd_hbm, wv_hbm, mixed_hbm, lp_ref,
    WG, WU, WD, WV, TOKS, X, GU, RB, PS, PR, H, RSS, RSR, OWN, MX, NB, SQS, SQR, L, LR,
    TG, ST, SR, send_sem, recv_sem, local_sem,
):
    z = lax.axis_index("grid")
    r = lax.axis_index("row")
    p = lax.axis_index("rep")
    own_rows = tok_hbm.shape[0]
    wave_rows = own_rows // 2
    chunk = wave_rows * 2
    quarter = chunk // 4
    dc = wg_hbm.shape[0]
    ff = wg_hbm.shape[1]
    vocab = wv_hbm.shape[0]
    width = 4 * dc

    row_peer = {"grid": z, "row": 1 - r, "rep": p}
    x_peer = {"grid": z, "row": r, "rep": 1 - p}

    def pal(s):
        return (z, z + 1 - 2 * lax.rem(z, 2), lax.rem(z + 2, RING), RING - 1 - z)[s]

    near = 1 + lax.rem(z, 2)
    far = jnp.where(z < RING // 2, RING - 1, 0)
    inner = jnp.where(z < RING // 2, RING // 2, RING // 2 - 1)
    turn = (z, near, 6 - z - near - far, far)
    targets = (pal(1), inner, far)
    at_end = jnp.logical_or(z == 0, z == RING - 1)
    inside = jnp.logical_and(z > 0, z < RING - 1)

    def at_grid(there):
        return {"grid": there, "row": r, "rep": p}

    sems = Sems(send_sem, recv_sem)

    def remote(src, dst, sem, device, landing=None):
        landing = sem if landing is None else landing
        return pltpu.make_async_remote_copy(
            src_ref=src, dst_ref=dst, send_sem=send_sem.at[sem], recv_sem=recv_sem.at[landing],
            device_id=device, device_id_type=MESH,
        )

    def to_chip(block, sem, there):
        return remote(block, block, sem + there, at_grid(there), sem + z)

    open_sends = {}

    def send(src, dst, sem, device):
        copy = remote(src, dst, sem, device)
        copy.start()
        open_sends[sem] = copy

    def sent(sem):
        open_sends.pop(sem).wait_send()

    def arrived(dst, sem):
        remote(dst, dst, sem, row_peer).wait_recv()

    loads = []

    def load(src, dst, n):
        copy = pltpu.make_async_copy(src, dst, local_sem.at[n])
        copy.start()
        loads.append(copy)
        return copy

    tok_loads = []
    for w in range(2):
        rows = pl.ds(w * wave_rows, wave_rows)
        theirs = pl.ds(pl.multiple_of((1 - p) * dc, dc), dc)
        mine = pl.ds(pl.multiple_of(p * dc, dc), dc)
        tok_loads.append((
            load(tok_hbm.at[rows, theirs], TOKS.at[w], 2 * w),
            load(tok_hbm.at[rows, mine], X.at[z, w, p], 2 * w + 1),
        ))
    wg_load = load(wg_hbm, WG, 4)
    wu_load = load(wu_hbm, WU, 5)
    wd_load = load(wd_hbm, WD, 6)
    wv_load = load(wv_hbm, WV, 7)

    barrier = pltpu.get_barrier_semaphore()
    for s in range(RING):
        for dr in range(2):
            for dp in range(2):
                if s or dr or dp:
                    pl.semaphore_signal(
                        barrier, inc=1,
                        device_id={"grid": lax.rem(z + s, RING), "row": lax.rem(r + dr, 2), "rep": lax.rem(p + dp, 2)},
                        device_id_type=MESH,
                    )
    pl.semaphore_wait(barrier, 4 * RING - 1)

    tok_x = [sems.take() for _ in range(2)]
    tok_z = [sems.take(RING) for _ in range(2)]
    for w in range(2):
        tok_loads[w][0].wait()
        send(TOKS.at[w], X.at[z, w, p], tok_x[w], x_peer)

    def take_tokens(w):
        tok_loads[w][1].wait()
        arrived(X.at[z, w, 1 - p], tok_x[w])

    def spread_tokens(w, which):
        for n in which:
            copy = to_chip(X.at[z, w], tok_z[w], targets[n])
            copy.start()
            open_sends["tokens", w, n] = copy

    n_chunks = 2 * RING
    order = [(0, s) for s in range(RING)] + [(1, s) for s in (1, 2, 3, 0)]
    dd = [[sems.take() for _ in range(2)] for _ in range(n_chunks)]
    xp = [sems.take() for _ in range(n_chunks)]
    xh = [sems.take() for _ in range(n_chunks)]
    dh = [sems.take() for _ in range(n_chunks)]
    df = [sems.take() for _ in range(n_chunks)]
    rs = [sems.take(RING) for _ in range(2)]

    def gate_up(c):
        w, s = order[c]
        zo = turn[s]
        slot = c % 2
        if s:
            arrived(X.at[zo, w], tok_z[w] + zo)
        for g, weight in enumerate((WG, WU)):
            if c >= 2:
                sent(dd[c - 2][g])

            def step(cols):
                x = X[zo, w].reshape(chunk, dc)
                part = jnp.dot(x, weight[:, cols], preferred_element_type=F32)
                for a in range(2):
                    for b in range(2):
                        at = (2 * a + b) * quarter
                        GU[slot, a, g, b, :, cols] = part[at : at + quarter]

            over_tiles(ff, step, GATE_TILE)
            send(GU.at[slot, 1 - r, g], RB.at[slot, g], dd[c][g], row_peer)

    def sum_rows(c):
        slot = c % 2
        if c >= 2:
            sent(xp[c - 2])
        if c >= 4:
            sent(df[c - 4])
        for g in range(2):
            arrived(RB.at[slot, g], dd[c][g])

            def step(cols):
                PS[slot, g, :, cols] = (
                    GU[slot, r, g, 1 - p, :, cols] + RB[slot, g, 1 - p, :, cols]
                ).astype(BF16)
                GU[slot, r, g, p, :, cols] = GU[slot, r, g, p, :, cols] + RB[slot, g, p, :, cols]

            over_tiles(ff, step)
        send(PS.at[slot], PR.at[c % 4], xp[c], x_peer)

    def activate(c):
        slot = c % 2
        hs = c % 4
        arrived(PR.at[hs], xp[c])
        if c >= 4:
            sent(xh[c - 4])
            sent(dh[c - 4])

        def step(cols):
            gate = GU[slot, r, 0, p, :, cols] + PR[hs, 0, :, cols].astype(F32)
            up_value = GU[slot, r, 1, p, :, cols] + PR[hs, 1, :, cols].astype(F32)
            hidden = gate / (1.0 + jnp.exp(-gate)) * up_value
            H[hs, r, p, :, cols] = hidden.astype(BF16)

        over_tiles(ff, step)
        send(H.at[hs, r, p], H.at[hs, r, p], xh[c], x_peer)
        send(H.at[hs, r, p], H.at[hs, r, p], dh[c], row_peer)

    def pass_on(c):
        hs = c % 4
        arrived(H.at[hs, r, 1 - p], xh[c])
        send(H.at[hs, r, 1 - p], H.at[hs, r, 1 - p], df[c], row_peer)

    def project(c):
        w, s = order[c]
        hs = c % 4
        arrived(H.at[hs, 1 - r, p], dh[c])
        arrived(H.at[hs, 1 - r, 1 - p], df[c])

        def step(cols):
            h = H[hs].reshape(chunk, ff)
            part = jnp.dot(h, WD[:, cols], preferred_element_type=F32)
            if s:
                RSS[w, s - 1, :, cols] = part.astype(BF16)
            else:
                OWN[w, :, cols] = part

        over_tiles(dc, step, PROJECT_TILE)
        if s:
            there = turn[s]
            copy = remote(RSS.at[w, s - 1], RSR.at[w, z], rs[w] + there, at_grid(there), rs[w] + z)
            copy.start()
            open_sends["sums", w, s] = copy

    def finish_rows(w):
        for there in turn[1:]:
            arrived(RSR.at[w, there], rs[w] + there)

        def step(cols):
            total = OWN[w, :, cols]
            for there in turn[1:]:
                total = total + RSR[w, there, :, cols].astype(F32)
            own = X[z, w, :, :, cols].reshape(chunk, cols.size).astype(F32)
            MX[z, w, p, :, cols] = (own + total).astype(BF16)

        over_tiles(dc, step)

    gz = [sems.take(RING) for _ in range(2)]
    hk = [sems.take() for _ in range(2)]
    gx = [[sems.take() for _ in range(RING)] for _ in range(2)]

    def gather_z(w, there):
        return to_chip(MX.at[z, w, p], gz[w], there)

    def start_gather(w):
        gather_z(w, targets[0]).start()
        gather_z(w, targets[1]).start()

        @pl.when(inside)
        def _():
            gather_z(w, far).start()

    def outward(w):
        block = MX.at[far, w, p]
        return remote(block, block, hk[w], at_grid(pal(1)), gz[w] + far)

    def hand_on(w):
        @pl.when(inside)
        def _():
            arrived(MX.at[far, w, p], gz[w] + far)
            outward(w).start()

    def drain_gather(w):
        gather_z(w, targets[0]).wait_send()
        gather_z(w, targets[1]).wait_send()

        @pl.when(inside)
        def _():
            gather_z(w, far).wait_send()
            outward(w).wait_send()

    def begin_first(ready):
        @pl.when(ready)
        def _():
            finish_rows(0)
            start_gather(0)

    def share(w, n):
        zb = sources[n]
        block = MX.at[zb, w, p]
        if n == RING - 1:
            @pl.when(at_end)
            def _():
                arrived(block, gz[w] + zb)
        elif n:
            arrived(block, gz[w] + zb)
        send(block, block, gx[w][n], x_peer)

    def shared(w, n):
        arrived(MX.at[sources[n], w, 1 - p], gx[w][n])

    sources = (z,) + targets

    take_tokens(0)
    spread_tokens(0, (0, 1, 2))
    wg_load.wait()
    wu_load.wait()
    gate_up(0)
    sum_rows(0)
    gate_up(1)
    sum_rows(1)
    take_tokens(1)
    spread_tokens(1, (0, 1))
    for i in range(n_chunks + 1):
        if i < n_chunks:
            activate(i)
        if i == n_chunks - 1:
            share(0, 0)
        if i + 2 < n_chunks:
            gate_up(i + 2)
        if i >= 1:
            pass_on(i - 1)
        if i + 2 < n_chunks:
            sum_rows(i + 2)
        if i == 1:
            wd_load.wait()
        if i == n_chunks:
            hand_on(0)
        if i >= 1:
            project(i - 1)
        if i == n_chunks - 1:
            share(0, 1)
        if i == 0:
            spread_tokens(1, (2,))
        if i == 4:
            begin_first(inside)
        if i == 5:
            begin_first(at_end)
    finish_rows(1)
    start_gather(1)
    share(0, 2)
    share(0, 3)
    share(1, 0)

    sq = [sems.take() for _ in range(n_chunks)]
    lg = [[sems.take() for _ in range(2)] for _ in range(2)]
    half = vocab // 2
    rows_tile = max(t for t in range(16, TILE + 1, 16) if half % t == 0)
    hop = half // 32 * 16
    big_tile = half - hop
    here = lax.div(z, 2)
    there = 1 - here

    def squares(k, zb, w):
        def part(h):
            v = MX[zb, w, h].astype(F32)
            return jnp.sum(v * v, axis=1, keepdims=True)

        SQS[k] = jnp.broadcast_to(part(0) + part(1), (chunk, LANES))
        send(SQS.at[k], SQR.at[k], sq[k], row_peer)

    def normalise(k, zb, w):
        arrived(SQR.at[k], sq[k])
        scale = lax.rsqrt((SQS[k] + SQR[k])[:, :1] / width + 1e-05)
        for h in range(2):
            cols = slice(h * dc, (h + 1) * dc)
            v = MX[zb, w, h].astype(F32) * scale * gain_ref[:, cols]
            NB[lax.div(zb, 2), lax.rem(zb, 2), :, cols] = v.astype(BF16)

    def logits_half(side, group):
        def step(n, carry):
            at = pl.multiple_of(n * hop, 16)
            rows = pl.ds(pl.multiple_of(side * half + at, 16), big_tile)
            x = NB[...] if group is None else NB[group]
            x = x.reshape(-1, 2 * dc)
            part = lax.dot_general(
                WV[rows, :], x, (((1,), (1,)), ((), ())), preferred_element_type=F32
            )
            if group is None:
                for g in range(2):
                    L[g, side, pl.ds(at, big_tile)] = part[:, g * LANES : (g + 1) * LANES]
            else:
                L[group, side, pl.ds(at, big_tile)] = part
            return carry

        lax.fori_loop(0, 2, step, 0)

    def exchange(w, n, group):
        send(L.at[group, 1 - r], LR.at[w, group], lg[w][n], row_peer)

    row_start = (z * 2 + p) * vocab + r * half

    def stats(w, n, group):
        arrived(LR.at[w, group], lg[w][n])
        step_rows = rows_tile
        steps = half // step_rows

        def add(i, top):
            rows = pl.ds(pl.multiple_of(i * step_rows, 8), step_rows)
            t = L[group, r, rows] + LR[w, group, rows]
            L[group, r, rows] = t
            return jnp.maximum(top, jnp.max(t.reshape(-1, 8, LANES), axis=0))

        top = lax.fori_loop(0, steps, add, jnp.full((8, LANES), -jnp.inf, F32))
        top = jnp.max(top, axis=0, keepdims=True)
        target = TG[w, group, 0:1] - row_start

        def count(i, carry):
            total, picked = carry
            rows = pl.ds(pl.multiple_of(i * step_rows, 8), step_rows)
            t = L[group, r, rows]
            ids = lax.broadcasted_iota(jnp.int32, t.shape, 0) + i * step_rows
            e = jnp.exp(t - top)
            hit = jnp.where(ids == target, t, 0.0)
            return (
                total + jnp.sum(e.reshape(-1, 8, LANES), axis=0),
                picked + jnp.sum(hit.reshape(-1, 8, LANES), axis=0),
            )

        zero = jnp.zeros((8, LANES), F32)
        total, picked = lax.fori_loop(0, steps, count, (zero, zero))
        ST[group, 4 * w : 4 * w + 1] = top
        ST[group, 4 * w + 1 : 4 * w + 2] = jnp.sum(total, axis=0, keepdims=True)
        ST[group, 4 * w + 2 : 4 * w + 3] = jnp.sum(picked, axis=0, keepdims=True)

    lane = lax.broadcasted_iota(jnp.int32, (8, LANES), 1)
    ST[...] = jnp.zeros_like(ST)
    for g in range(2):
        for w in range(2):
            line = None
            for spot in range(4):
                source = 2 * (spot % 2) + w
                ids = jnp.broadcast_to(tgt_ref[2 * g + spot // 2], (8, LANES))
                ids = pltpu.roll(ids, ((spot - source) * wave_rows) % LANES, 1)
                line = ids if line is None else jnp.where(lane >= spot * wave_rows, ids, line)
            TG[w, g] = line

    for n in range(RING):
        shared(0, n)
        squares(n, sources[n], 0)
    wv_load.wait()
    for n in range(RING):
        normalise(n, sources[n], 0)
    share(1, 1)
    logits_half(1 - r, None)
    for g in range(2):
        exchange(0, g, g)
    hand_on(1)
    share(1, 2)
    logits_half(r, None)
    for n in range(2):
        shared(1, n)
        squares(RING + n, sources[n], 1)
    outs = []
    for w in range(2):
        for h in range(2):
            rows = pl.ds(pl.multiple_of(p * wave_rows, wave_rows), wave_rows)
            copy = pltpu.make_async_copy(
                MX.at[z, w, h, rows],
                mixed_hbm.at[pl.ds(w * wave_rows, wave_rows), pl.ds(h * dc, dc)],
                local_sem.at[2 * w + h],
            )
            copy.start()
            outs.append(copy)

    for g in range(2):
        stats(0, g, g)
    for g in range(2):
        sent(lg[0][g])
    for n in range(2):
        normalise(RING + n, sources[n], 1)
    logits_half(1 - r, here)
    exchange(1, 0, here)
    share(1, 3)
    logits_half(r, here)
    for n in (2, 3):
        shared(1, n)
        squares(RING + n, sources[n], 1)
    stats(1, 0, here)
    for n in (2, 3):
        normalise(RING + n, sources[n], 1)
    logits_half(1 - r, there)
    exchange(1, 1, there)
    logits_half(r, there)
    stats(1, 1, there)

    n_all = 4 * RING
    st = sems.take(n_all)
    base = sems.take(n_all)
    me = (z * 2 + r) * 2 + p

    def others():
        for s in (3, 2, 1, 0):
            for dr in range(2):
                for dp in range(2):
                    if s or dr or dp:
                        yield s, dr, dp

    def figures(s, dr, dp):
        device = {"grid": pal(s), "row": lax.rem(r + dr, 2), "rep": lax.rem(p + dp, 2)}
        return pltpu.make_async_remote_copy(
            src_ref=ST.at[lax.div(pal(s), 2)], dst_ref=SR.at[me],
            send_sem=send_sem.at[st + 4 * s + 2 * dr + dp], recv_sem=recv_sem.at[base + me],
            device_id=device, device_id_type=MESH,
        )

    for other in others():
        figures(*other).start()
    SR[me] = ST[here]
    for s, dr, dp in others():
        who = (pal(s) * 2 + lax.rem(r + dr, 2)) * 2 + lax.rem(p + dp, 2)
        arrived(SR.at[who], base + who)

    lines = []
    for w in range(2):
        top = SR[0, 4 * w : 4 * w + 1]
        for n in range(1, n_all):
            top = jnp.maximum(top, SR[n, 4 * w : 4 * w + 1])
        total = jnp.zeros_like(top)
        picked = jnp.zeros_like(top)
        for n in range(n_all):
            total = total + SR[n, 4 * w + 1 : 4 * w + 2] * jnp.exp(SR[n, 4 * w : 4 * w + 1] - top)
            picked = picked + SR[n, 4 * w + 2 : 4 * w + 3]
        lines.append(jnp.broadcast_to(picked - top - jnp.log(total), (8, LANES)))
    spot = lax.rem(z, 2) * 2 + p
    result = jnp.zeros((8, LANES), F32)
    for k in range(4):
        a = pltpu.roll(lines[0], (-k * wave_rows) % LANES, 1)
        b = pltpu.roll(lines[1], ((1 - k) * wave_rows) % LANES, 1)
        result = jnp.where(spot == k, jnp.where(lane < wave_rows, a, b), result)
    lp_ref[...] = result[0:1, : lp_ref.shape[1]]

    for other in others():
        figures(*other).wait_send()
    for w in range(2):
        drain_gather(w)
    for sem in list(open_sends):
        sent(sem)
    for copy in outs:
        copy.wait()


N_SEMS = 160


def block(tokens, target_tokens, gate_weight, up_weight, down_weight, norm_gain, vocab_weight):
    own_rows, half_width = tokens.shape
    wave_rows = own_rows // 2
    chunk = 2 * wave_rows
    quarter = chunk // 4
    dc, ff = gate_weight.shape
    vocab = vocab_weight.shape[1]
    vmem = pltpu.VMEM
    any_space = pl.BlockSpec(memory_space=pl.ANY)
    in_vmem = pl.BlockSpec(memory_space=pltpu.VMEM)
    targets = target_tokens.reshape(RING, 1, 2 * own_rows)
    gain = norm_gain.reshape(1, half_width)
    mixed, logprob = pl.pallas_call(
        block_kernel,
        out_shape=(
            jax.ShapeDtypeStruct((own_rows, half_width), BF16),
            jax.ShapeDtypeStruct((1, own_rows), F32),
        ),
        in_specs=[any_space, in_vmem, in_vmem, any_space, any_space, any_space, any_space],
        out_specs=(any_space, in_vmem),
        scratch_shapes=[
            vmem((dc, ff), BF16),
            vmem((dc, ff), BF16),
            vmem((ff, dc), BF16),
            vmem((vocab, half_width), BF16),
            vmem((2, wave_rows, dc), BF16),
            vmem((RING, 2, 2, wave_rows, dc), BF16),
            vmem((2, 2, 2, 2, quarter, ff), F32),
            vmem((2, 2, 2, quarter, ff), F32),
            vmem((2, 2, quarter, ff), BF16),
            vmem((4, 2, quarter, ff), BF16),
            vmem((4, 2, 2, quarter, ff), BF16),
            vmem((2, RING - 1, chunk, dc), BF16),
            vmem((2, RING, chunk, dc), BF16),
            vmem((2, chunk, dc), F32),
            vmem((RING, 2, 2, chunk, dc), BF16),
            vmem((2, 2, chunk, half_width), BF16),
            vmem((2 * RING, chunk, LANES), F32),
            vmem((2 * RING, chunk, LANES), F32),
            vmem((2, 2, vocab // 2, LANES), F32),
            vmem((2, 2, vocab // 2, LANES), F32),
            vmem((2, 2, 8, LANES), jnp.int32),
            vmem((2, 8, LANES), F32),
            vmem((4 * RING, 8, LANES), F32),
            pltpu.SemaphoreType.DMA((N_SEMS,)),
            pltpu.SemaphoreType.DMA((N_SEMS,)),
            pltpu.SemaphoreType.DMA((8,)),
        ],
        compiler_params=pltpu.CompilerParams(
            collective_id=0, has_side_effects=True, vmem_limit_bytes=67_043_328
        ),
        name="block",
    )(tokens, targets, gain, gate_weight, up_weight, down_weight, vocab_weight.T)
    return (mixed, logprob.reshape(own_rows))


def solution(mesh):
    in_specs = (
        P(("groups", "grid", "rep"), "row"),
        P("groups"),
        P(("row", "rep"), "grid"),
        P(("row", "rep"), "grid"),
        P("grid", ("row", "rep")),
        P("row"),
        P("row", ("grid", "rep")),
    )
    out_specs = (P(("groups", "grid", "rep"), "row"), P(("groups", "grid", "rep")))
    small = mesh.shape["row"] == 2 and mesh.shape["rep"] == 2 and mesh.shape["grid"] == RING
    return jax.shard_map(
        block if small else general,
        mesh=mesh,
        in_specs=in_specs,
        out_specs=out_specs,
        check_vma=False,
    )
```

```python
import jax
import jax.numpy as jnp
from jax import lax
from jax.experimental import pallas as pl
from jax.experimental.pallas import tpu as pltpu
from jax.sharding import PartitionSpec as P

F32 = jnp.float32
BF16 = jnp.bfloat16
MESH = pl.DeviceIdType.MESH
LANES = 128
TILE = 512
GATE_TILE = 1792
PROJECT_TILE = 1024
RING = 4


def pick_target(logits, targets, column_start):
    column_ids = column_start + lax.broadcasted_iota(jnp.int32, logits.shape, 1)
    return jnp.sum(jnp.where(column_ids == targets[:, None], logits, 0.0), axis=1)


def stats_all(logits, targets, column_start):
    picked = pick_target(logits, targets, column_start)
    row_top = lax.pmax(jnp.max(logits, axis=1), ("grid", "rep"))
    local_total = jnp.sum(jnp.exp(logits - row_top[:, None]), axis=1)
    row_total, target_logit = lax.psum((local_total, picked), ("grid", "rep"))
    return target_logit - row_top - jnp.log(row_total)


def general(tokens, target_tokens, gate_weight, up_weight, down_weight, norm_gain, vocab_weight):
    own_rows = tokens.shape[0]
    width = tokens.shape[1] * lax.axis_size("row")
    copy_rows = lax.all_gather(tokens, "grid", axis=0, tiled=True)
    gate_part = jnp.dot(
        copy_rows,
        lax.all_gather(gate_weight, "rep", axis=0, tiled=True),
        preferred_element_type=F32,
    )
    up_part = jnp.dot(
        copy_rows,
        lax.all_gather(up_weight, "rep", axis=0, tiled=True),
        preferred_element_type=F32,
    )
    gate_value, up_value = lax.psum((gate_part, up_part), "row")
    hidden = (jax.nn.silu(gate_value) * up_value).astype(BF16)
    down_full = lax.all_gather(down_weight, "rep", axis=1, tiled=True)
    branch_sum = lax.psum_scatter(
        jnp.dot(hidden, down_full, preferred_element_type=F32),
        "grid",
        scatter_dimension=0,
        tiled=True,
    )
    mixed = (tokens.astype(F32) + branch_sum).astype(BF16)
    held = lax.optimization_barrier(mixed).astype(F32)
    squares = lax.psum(jnp.sum(held * held, axis=1), "row")
    scale = lax.rsqrt(squares / width + 1e-05)
    normed = (held * scale[:, None] * norm_gain[None, :]).astype(BF16)
    partial_logits = jnp.dot(
        lax.all_gather(normed, ("grid", "rep"), axis=0, tiled=True),
        vocab_weight,
        preferred_element_type=F32,
    )
    logits = lax.psum(partial_logits, "row")
    block_index = lax.axis_index(("grid", "rep"))
    column_start = block_index * vocab_weight.shape[1]
    every_logprob = stats_all(logits, target_tokens, column_start)
    logprob = lax.dynamic_slice_in_dim(every_logprob, block_index * own_rows, own_rows, 0)
    return (mixed, logprob)


def tiles(width, tile=TILE):
    full = width // tile
    return full, width - full * tile


def over_tiles(width, step, tile=TILE):
    full, rest = tiles(width, tile)

    def one(n, carry):
        step(pl.ds(pl.multiple_of(n * tile, tile), tile))
        return carry

    if full == 1:
        step(pl.ds(0, tile))
    elif full:
        lax.fori_loop(0, full, one, 0)
    if rest:
        step(pl.ds(full * tile, rest))


class Sems:
    def __init__(self, send, recv):
        self.send, self.recv, self.used = send, recv, 0

    def take(self, count=1):
        first = self.used
        self.used += count
        return first


def block_kernel(
    tok_hbm, tgt_ref, gain_ref, wg_hbm, wu_hbm, wd_hbm, wv_hbm, mixed_hbm, lp_ref,
    WG, WU, WD, WV, TOKS, X, GU, RB, PS, PR, H, RSS, RSR, OWN, MX, NB, SQS, SQR, L, LR,
    TG, ST, SR, send_sem, recv_sem, local_sem,
):
    z = lax.axis_index("grid")
    r = lax.axis_index("row")
    p = lax.axis_index("rep")
    own_rows = tok_hbm.shape[0]
    wave_rows = own_rows // 2
    chunk = wave_rows * 2
    quarter = chunk // 4
    dc = wg_hbm.shape[0]
    ff = wg_hbm.shape[1]
    vocab = wv_hbm.shape[0]
    width = 4 * dc

    row_peer = {"grid": z, "row": 1 - r, "rep": p}
    x_peer = {"grid": z, "row": r, "rep": 1 - p}

    def pal(s):
        return (z, z + 1 - 2 * lax.rem(z, 2), lax.rem(z + 2, RING), RING - 1 - z)[s]

    near = 1 + lax.rem(z, 2)
    far = jnp.where(z < RING // 2, RING - 1, 0)
    inner = jnp.where(z < RING // 2, RING // 2, RING // 2 - 1)
    turn = (z, near, 6 - z - near - far, far)
    targets = (pal(1), inner, far)
    at_end = jnp.logical_or(z == 0, z == RING - 1)
    inside = jnp.logical_and(z > 0, z < RING - 1)

    def at_grid(there):
        return {"grid": there, "row": r, "rep": p}

    sems = Sems(send_sem, recv_sem)

    def remote(src, dst, sem, device, landing=None):
        landing = sem if landing is None else landing
        return pltpu.make_async_remote_copy(
            src_ref=src, dst_ref=dst, send_sem=send_sem.at[sem], recv_sem=recv_sem.at[landing],
            device_id=device, device_id_type=MESH,
        )

    def to_chip(block, sem, there):
        return remote(block, block, sem + there, at_grid(there), sem + z)

    open_sends = {}

    def send(src, dst, sem, device):
        copy = remote(src, dst, sem, device)
        copy.start()
        open_sends[sem] = copy

    def sent(sem):
        open_sends.pop(sem).wait_send()

    def arrived(dst, sem):
        remote(dst, dst, sem, row_peer).wait_recv()

    loads = []

    def load(src, dst, n):
        copy = pltpu.make_async_copy(src, dst, local_sem.at[n])
        copy.start()
        loads.append(copy)
        return copy

    tok_loads = []
    for w in range(2):
        rows = pl.ds(w * wave_rows, wave_rows)
        theirs = pl.ds(pl.multiple_of((1 - p) * dc, dc), dc)
        mine = pl.ds(pl.multiple_of(p * dc, dc), dc)
        tok_loads.append((
            load(tok_hbm.at[rows, theirs], TOKS.at[w], 2 * w),
            load(tok_hbm.at[rows, mine], X.at[z, w, p], 2 * w + 1),
        ))
    wg_load = load(wg_hbm, WG, 4)
    wu_load = load(wu_hbm, WU, 5)
    wd_load = load(wd_hbm, WD, 6)
    wv_load = load(wv_hbm, WV, 7)

    barrier = pltpu.get_barrier_semaphore()
    for s in range(RING):
        for dr in range(2):
            for dp in range(2):
                if s or dr or dp:
                    pl.semaphore_signal(
                        barrier, inc=1,
                        device_id={"grid": lax.rem(z + s, RING), "row": lax.rem(r + dr, 2), "rep": lax.rem(p + dp, 2)},
                        device_id_type=MESH,
                    )
    pl.semaphore_wait(barrier, 4 * RING - 1)

    tok_x = [sems.take() for _ in range(2)]
    tok_z = [sems.take(RING) for _ in range(2)]
    for w in range(2):
        tok_loads[w][0].wait()
        send(TOKS.at[w], X.at[z, w, p], tok_x[w], x_peer)

    def take_tokens(w):
        tok_loads[w][1].wait()
        arrived(X.at[z, w, 1 - p], tok_x[w])

    def tokens_to(w, n):
        return to_chip(X.at[z, w], tok_z[w], targets[n])

    def spread_tokens(w, from_middle, from_end):
        @pl.when(inside)
        def _():
            for n in from_middle:
                tokens_to(w, n).start()

        @pl.when(at_end)
        def _():
            for n in from_end:
                tokens_to(w, n).start()

    n_chunks = 2 * RING
    order = [(0, s) for s in range(RING)] + [(1, s) for s in (3, 1, 2, 0)]
    dd = [[sems.take() for _ in range(2)] for _ in range(n_chunks)]
    xp = [[sems.take() for _ in range(2)] for _ in range(n_chunks)]
    xh = [sems.take() for _ in range(n_chunks)]
    dh = [sems.take() for _ in range(n_chunks)]
    df = [sems.take() for _ in range(n_chunks)]
    rs = [sems.take(RING) for _ in range(2)]

    def gate_up(c):
        w, s = order[c]
        zo = turn[s]
        slot = c % 2
        if s:
            arrived(X.at[zo, w], tok_z[w] + zo)
        for g, weight in enumerate((WG, WU)):
            if c >= 2:
                sent(dd[c - 2][g])

            def step(cols):
                x = X[zo, w].reshape(chunk, dc)
                part = jnp.dot(x, weight[:, cols], preferred_element_type=F32)
                for a in range(2):
                    for b in range(2):
                        at = (2 * a + b) * quarter
                        GU[slot, a, g, b, :, cols] = part[at : at + quarter]

            over_tiles(ff, step, GATE_TILE)
            send(GU.at[slot, 1 - r, g], RB.at[slot, g], dd[c][g], row_peer)

    def sum_rows(c):
        slot = c % 2
        if c >= 4:
            sent(df[c - 4])
        for g in range(2):
            if c >= 2:
                sent(xp[c - 2][g])
            arrived(RB.at[slot, g], dd[c][g])

            def step(cols):
                PS[slot, g, :, cols] = (
                    GU[slot, r, g, 1 - p, :, cols] + RB[slot, g, 1 - p, :, cols]
                ).astype(BF16)
                GU[slot, r, g, p, :, cols] = GU[slot, r, g, p, :, cols] + RB[slot, g, p, :, cols]

            over_tiles(ff, step)
            send(PS.at[slot, g], PR.at[c % 4, g], xp[c][g], x_peer)

    def activate(c):
        slot = c % 2
        hs = c % 4
        for g in range(2):
            arrived(PR.at[hs, g], xp[c][g])
        if c >= 4:
            sent(xh[c - 4])
            sent(dh[c - 4])

        def step(cols):
            gate = GU[slot, r, 0, p, :, cols] + PR[hs, 0, :, cols].astype(F32)
            up_value = GU[slot, r, 1, p, :, cols] + PR[hs, 1, :, cols].astype(F32)
            hidden = gate / (1.0 + jnp.exp(-gate)) * up_value
            H[hs, r, p, :, cols] = hidden.astype(BF16)

        over_tiles(ff, step)
        send(H.at[hs, r, p], H.at[hs, r, p], xh[c], x_peer)
        send(H.at[hs, r, p], H.at[hs, r, p], dh[c], row_peer)

    def pass_on(c):
        hs = c % 4
        arrived(H.at[hs, r, 1 - p], xh[c])
        send(H.at[hs, r, 1 - p], H.at[hs, r, 1 - p], df[c], row_peer)

    def project(c):
        w, s = order[c]
        hs = c % 4
        arrived(H.at[hs, 1 - r, p], dh[c])
        arrived(H.at[hs, 1 - r, 1 - p], df[c])

        def step(cols):
            h = H[hs].reshape(chunk, ff)
            part = jnp.dot(h, WD[:, cols], preferred_element_type=F32)
            if s:
                RSS[w, s - 1, :, cols] = part.astype(BF16)
            else:
                OWN[w, :, cols] = part

        over_tiles(dc, step, PROJECT_TILE)
        if s:
            there = turn[s]
            copy = remote(RSS.at[w, s - 1], RSR.at[w, z], rs[w] + there, at_grid(there), rs[w] + z)
            copy.start()
            open_sends["sums", w, s] = copy

    def finish_rows(w):
        for there in turn[1:]:
            arrived(RSR.at[w, there], rs[w] + there)

        def step(cols):
            total = OWN[w, :, cols]
            for there in turn[1:]:
                total = total + RSR[w, there, :, cols].astype(F32)
            own = X[z, w, :, :, cols].reshape(chunk, cols.size).astype(F32)
            MX[z, w, p, :, cols] = (own + total).astype(BF16)

        over_tiles(dc, step)

    gz = [sems.take(RING) for _ in range(2)]
    hk = [sems.take(3) for _ in range(2)]
    gx = [[sems.take() for _ in range(RING)] for _ in range(2)]

    def gather_z(w, there):
        return to_chip(MX.at[z, w, p], gz[w], there)

    def start_gather(w):
        for there in targets[:2]:
            gather_z(w, there).start()

    def outward(w, n):
        zb = targets[n]
        block = MX.at[zb, w, p]
        return remote(block, block, hk[w] + n, at_grid(pal(1)), gz[w] + zb)

    def hand_on(w, n):
        @pl.when(inside)
        def _():
            arrived(MX.at[targets[n], w, p], gz[w] + targets[n])
            outward(w, n).start()

    def drain_gather(w):
        for there in targets[:2]:
            gather_z(w, there).wait_send()

        @pl.when(inside)
        def _():
            for n in (1, 2):
                outward(w, n).wait_send()

    def begin_first(ready):
        @pl.when(ready)
        def _():
            finish_rows(0)
            start_gather(0)

    def share(w, n, when_inside=True, when_at_end=True):
        zb = sources[n]
        block = MX.at[zb, w, p]
        copy = remote(block, block, gx[w][n], x_peer)
        open_sends["share", w, n] = copy
        if n < 2:
            if n == 1:
                arrived(block, gz[w] + zb)
            copy.start()
            return
        if when_inside:

            @pl.when(inside)
            def _():
                copy.start()

        if when_at_end:

            @pl.when(at_end)
            def _():
                arrived(block, gz[w] + zb)
                copy.start()

    def shared(w, n):
        arrived(MX.at[sources[n], w, 1 - p], gx[w][n])

    sources = (z,) + targets

    take_tokens(0)
    spread_tokens(0, (0, 1), ())
    wg_load.wait()
    wu_load.wait()
    gate_up(0)
    spread_tokens(0, (2,), (0,))
    sum_rows(0)
    gate_up(1)
    spread_tokens(0, (), (1, 2))
    sum_rows(1)
    take_tokens(1)
    for i in range(n_chunks + 1):
        if i < n_chunks:
            activate(i)
        if i == n_chunks - 2:
            hand_on(0, 1)
        if i == n_chunks - 1:
            share(0, 0)
        if i + 2 < n_chunks:
            gate_up(i + 2)
        if i >= 1:
            pass_on(i - 1)
        if i + 2 < n_chunks:
            sum_rows(i + 2)
        if i == 1:
            wd_load.wait()
        if i >= 1:
            project(i - 1)
        if i == n_chunks - 1:
            share(0, 1)
            hand_on(0, 2)
        if i == 0:
            spread_tokens(1, (2, 1), (2, 1))
        if i == 1:
            spread_tokens(1, (0,), (0,))
        if i == 4:
            begin_first(inside)
        if i == 6:
            begin_first(at_end)
    finish_rows(1)
    start_gather(1)
    share(0, 2)
    share(1, 0)
    share(0, 3)

    sq = [sems.take() for _ in range(n_chunks)]
    lg = [[sems.take(2) for _ in range(2)] for _ in range(2)]
    half = vocab // 2
    rows_tile = max(t for t in range(16, TILE + 1, 16) if half % t == 0)
    hop = half // 32 * 16
    big_tile = half - hop
    here = lax.div(z, 2)

    def squares(k, zb, w):
        def part(h):
            v = MX[zb, w, h].astype(F32)
            return jnp.sum(v * v, axis=1, keepdims=True)

        SQS[k] = jnp.broadcast_to(part(0) + part(1), (chunk, LANES))
        send(SQS.at[k], SQR.at[k], sq[k], row_peer)

    def normalise(k, zb, w):
        arrived(SQR.at[k], sq[k])
        scale = lax.rsqrt((SQS[k] + SQR[k])[:, :1] / width + 1e-05)
        for h in range(2):
            cols = slice(h * dc, (h + 1) * dc)
            v = MX[zb, w, h].astype(F32) * scale * gain_ref[:, cols]
            NB[lax.div(zb, 2), lax.rem(zb, 2), :, cols] = v.astype(BF16)

    def logits_half(side, first_tile=0, last_tile=2):
        def step(n, carry):
            at = pl.multiple_of(n * hop, 16)
            rows = pl.ds(pl.multiple_of(side * half + at, 16), big_tile)
            x = NB[...].reshape(-1, 2 * dc)
            part = lax.dot_general(
                WV[rows, :], x, (((1,), (1,)), ((), ())), preferred_element_type=F32
            )
            for g in range(2):
                L[g, side, pl.ds(at, big_tile)] = part[:, g * LANES : (g + 1) * LANES]
            return carry

        lax.fori_loop(first_tile, last_tile, step, 0)

    def exchange(w, piece):
        rows = (pl.ds(0, hop), pl.ds(hop, big_tile))[piece]
        for g in range(2):
            send(L.at[g, 1 - r, rows], LR.at[w, g, rows], lg[w][g] + piece, row_peer)

    row_start = (z * 2 + p) * vocab + r * half

    def stats(w, group):
        arrived(LR.at[w, group, pl.ds(0, hop)], lg[w][group])
        arrived(LR.at[w, group, pl.ds(hop, big_tile)], lg[w][group] + 1)
        step_rows = rows_tile
        steps = half // step_rows

        def add(i, top):
            rows = pl.ds(pl.multiple_of(i * step_rows, 8), step_rows)
            t = L[group, r, rows] + LR[w, group, rows]
            L[group, r, rows] = t
            return jnp.maximum(top, jnp.max(t.reshape(-1, 8, LANES), axis=0))

        top = lax.fori_loop(0, steps, add, jnp.full((8, LANES), -jnp.inf, F32))
        top = jnp.max(top, axis=0, keepdims=True)
        target = TG[w, group, 0:1] - row_start

        def count(i, carry):
            total, picked = carry
            rows = pl.ds(pl.multiple_of(i * step_rows, 8), step_rows)
            t = L[group, r, rows]
            ids = lax.broadcasted_iota(jnp.int32, t.shape, 0) + i * step_rows
            e = jnp.exp(t - top)
            hit = jnp.where(ids == target, t, 0.0)
            return (
                total + jnp.sum(e.reshape(-1, 8, LANES), axis=0),
                picked + jnp.sum(hit.reshape(-1, 8, LANES), axis=0),
            )

        zero = jnp.zeros((8, LANES), F32)
        total, picked = lax.fori_loop(0, steps, count, (zero, zero))
        ST[group, 4 * w : 4 * w + 1] = top
        ST[group, 4 * w + 1 : 4 * w + 2] = jnp.sum(total, axis=0, keepdims=True)
        ST[group, 4 * w + 2 : 4 * w + 3] = jnp.sum(picked, axis=0, keepdims=True)

    lane = lax.broadcasted_iota(jnp.int32, (8, LANES), 1)
    ST[...] = jnp.zeros_like(ST)
    for g in range(2):
        for w in range(2):
            line = None
            for spot in range(4):
                source = 2 * (spot % 2) + w
                ids = jnp.broadcast_to(tgt_ref[2 * g + spot // 2], (8, LANES))
                ids = pltpu.roll(ids, ((spot - source) * wave_rows) % LANES, 1)
                line = ids if line is None else jnp.where(lane >= spot * wave_rows, ids, line)
            TG[w, g] = line

    for n in range(RING):
        shared(0, n)
        squares(n, sources[n], 0)
        if n == 1:
            share(1, 1)
        if n == 2:
            hand_on(1, 1)
            share(1, 2, when_at_end=False)
            hand_on(1, 2)
            share(1, 3, when_at_end=False)
    wv_load.wait()
    for n in range(RING):
        normalise(n, sources[n], 0)
    logits_half(1 - r)
    exchange(0, 0)
    exchange(0, 1)
    share(1, 2, when_inside=False)
    share(1, 3, when_inside=False)
    logits_half(r)
    for n in range(2):
        shared(1, n)
        squares(RING + n, sources[n], 1)
    outs = []
    for w in range(2):
        for h in range(2):
            rows = pl.ds(pl.multiple_of(p * wave_rows, wave_rows), wave_rows)
            copy = pltpu.make_async_copy(
                MX.at[z, w, h, rows],
                mixed_hbm.at[pl.ds(w * wave_rows, wave_rows), pl.ds(h * dc, dc)],
                local_sem.at[2 * w + h],
            )
            copy.start()
            outs.append(copy)

    for g in range(2):
        stats(0, g)
    for g in range(2):
        for piece in range(2):
            sent(lg[0][g] + piece)
    for n in (2, 3):
        shared(1, n)
        squares(RING + n, sources[n], 1)
    for n in range(RING):
        normalise(RING + n, sources[n], 1)
    for piece in range(2):
        logits_half(1 - r, piece, piece + 1)
        exchange(1, piece)
    logits_half(r)
    for g in range(2):
        stats(1, g)

    n_all = 4 * RING
    st = sems.take(n_all)
    base = sems.take(n_all)
    me = (z * 2 + r) * 2 + p

    def others():
        for s in (3, 2, 1, 0):
            for dr in range(2):
                for dp in range(2):
                    if s or dr or dp:
                        yield s, dr, dp

    def figures(s, dr, dp):
        device = {"grid": pal(s), "row": lax.rem(r + dr, 2), "rep": lax.rem(p + dp, 2)}
        return pltpu.make_async_remote_copy(
            src_ref=ST.at[lax.div(pal(s), 2)], dst_ref=SR.at[me],
            send_sem=send_sem.at[st + 4 * s + 2 * dr + dp], recv_sem=recv_sem.at[base + me],
            device_id=device, device_id_type=MESH,
        )

    for other in others():
        figures(*other).start()
    SR[me] = ST[here]
    for s, dr, dp in others():
        who = (pal(s) * 2 + lax.rem(r + dr, 2)) * 2 + lax.rem(p + dp, 2)
        arrived(SR.at[who], base + who)

    lines = []
    for w in range(2):
        top = SR[0, 4 * w : 4 * w + 1]
        for n in range(1, n_all):
            top = jnp.maximum(top, SR[n, 4 * w : 4 * w + 1])
        total = jnp.zeros_like(top)
        picked = jnp.zeros_like(top)
        for n in range(n_all):
            total = total + SR[n, 4 * w + 1 : 4 * w + 2] * jnp.exp(SR[n, 4 * w : 4 * w + 1] - top)
            picked = picked + SR[n, 4 * w + 2 : 4 * w + 3]
        lines.append(jnp.broadcast_to(picked - top - jnp.log(total), (8, LANES)))
    spot = lax.rem(z, 2) * 2 + p
    result = jnp.zeros((8, LANES), F32)
    for k in range(4):
        a = pltpu.roll(lines[0], (-k * wave_rows) % LANES, 1)
        b = pltpu.roll(lines[1], ((1 - k) * wave_rows) % LANES, 1)
        result = jnp.where(spot == k, jnp.where(lane < wave_rows, a, b), result)
    lp_ref[...] = result[0:1, : lp_ref.shape[1]]

    for other in others():
        figures(*other).wait_send()
    for w in range(2):
        for n in range(3):
            tokens_to(w, n).wait_send()
        drain_gather(w)
    for sem in list(open_sends):
        sent(sem)
    for copy in outs:
        copy.wait()


N_SEMS = 160


def block(tokens, target_tokens, gate_weight, up_weight, down_weight, norm_gain, vocab_weight):
    own_rows, half_width = tokens.shape
    wave_rows = own_rows // 2
    chunk = 2 * wave_rows
    quarter = chunk // 4
    dc, ff = gate_weight.shape
    vocab = vocab_weight.shape[1]
    vmem = pltpu.VMEM
    any_space = pl.BlockSpec(memory_space=pl.ANY)
    in_vmem = pl.BlockSpec(memory_space=pltpu.VMEM)
    targets = target_tokens.reshape(RING, 1, 2 * own_rows)
    gain = norm_gain.reshape(1, half_width)
    mixed, logprob = pl.pallas_call(
        block_kernel,
        out_shape=(
            jax.ShapeDtypeStruct((own_rows, half_width), BF16),
            jax.ShapeDtypeStruct((1, own_rows), F32),
        ),
        in_specs=[any_space, in_vmem, in_vmem, any_space, any_space, any_space, any_space],
        out_specs=(any_space, in_vmem),
        scratch_shapes=[
            vmem((dc, ff), BF16),
            vmem((dc, ff), BF16),
            vmem((ff, dc), BF16),
            vmem((vocab, half_width), BF16),
            vmem((2, wave_rows, dc), BF16),
            vmem((RING, 2, 2, wave_rows, dc), BF16),
            vmem((2, 2, 2, 2, quarter, ff), F32),
            vmem((2, 2, 2, quarter, ff), F32),
            vmem((2, 2, quarter, ff), BF16),
            vmem((4, 2, quarter, ff), BF16),
            vmem((4, 2, 2, quarter, ff), BF16),
            vmem((2, RING - 1, chunk, dc), BF16),
            vmem((2, RING, chunk, dc), BF16),
            vmem((2, chunk, dc), F32),
            vmem((RING, 2, 2, chunk, dc), BF16),
            vmem((2, 2, chunk, half_width), BF16),
            vmem((2 * RING, chunk, LANES), F32),
            vmem((2 * RING, chunk, LANES), F32),
            vmem((2, 2, vocab // 2, LANES), F32),
            vmem((2, 2, vocab // 2, LANES), F32),
            vmem((2, 2, 8, LANES), jnp.int32),
            vmem((2, 8, LANES), F32),
            vmem((4 * RING, 8, LANES), F32),
            pltpu.SemaphoreType.DMA((N_SEMS,)),
            pltpu.SemaphoreType.DMA((N_SEMS,)),
            pltpu.SemaphoreType.DMA((8,)),
        ],
        compiler_params=pltpu.CompilerParams(
            collective_id=0, has_side_effects=True, vmem_limit_bytes=67_043_328
        ),
        name="block",
    )(tokens, targets, gain, gate_weight, up_weight, down_weight, vocab_weight.T)
    return (mixed, logprob.reshape(own_rows))


def solution(mesh):
    in_specs = (
        P(("groups", "grid", "rep"), "row"),
        P("groups"),
        P(("row", "rep"), "grid"),
        P(("row", "rep"), "grid"),
        P("grid", ("row", "rep")),
        P("row"),
        P("row", ("grid", "rep")),
    )
    out_specs = (P(("groups", "grid", "rep"), "row"), P(("groups", "grid", "rep")))
    small = mesh.shape["row"] == 2 and mesh.shape["rep"] == 2 and mesh.shape["grid"] == RING
    return jax.shard_map(
        block if small else general,
        mesh=mesh,
        in_specs=in_specs,
        out_specs=out_specs,
        check_vma=False,
    )
```

```python
import jax
import jax.numpy as jnp
from jax import lax
from jax.experimental import pallas as pl
from jax.experimental.pallas import tpu as pltpu
from jax.sharding import PartitionSpec as P

F32 = jnp.float32
BF16 = jnp.bfloat16
MESH = pl.DeviceIdType.MESH
LANES = 128
TILE = 512
GATE_TILE = 1792
PROJECT_TILE = 1024
RING = 4


def pick_target(logits, targets, column_start):
    column_ids = column_start + lax.broadcasted_iota(jnp.int32, logits.shape, 1)
    return jnp.sum(jnp.where(column_ids == targets[:, None], logits, 0.0), axis=1)


def stats_all(logits, targets, column_start):
    picked = pick_target(logits, targets, column_start)
    row_top = lax.pmax(jnp.max(logits, axis=1), ("grid", "rep"))
    local_total = jnp.sum(jnp.exp(logits - row_top[:, None]), axis=1)
    row_total, target_logit = lax.psum((local_total, picked), ("grid", "rep"))
    return target_logit - row_top - jnp.log(row_total)


def general(tokens, target_tokens, gate_weight, up_weight, down_weight, norm_gain, vocab_weight):
    own_rows = tokens.shape[0]
    width = tokens.shape[1] * lax.axis_size("row")
    copy_rows = lax.all_gather(tokens, "grid", axis=0, tiled=True)
    gate_part = jnp.dot(
        copy_rows,
        lax.all_gather(gate_weight, "rep", axis=0, tiled=True),
        preferred_element_type=F32,
    )
    up_part = jnp.dot(
        copy_rows,
        lax.all_gather(up_weight, "rep", axis=0, tiled=True),
        preferred_element_type=F32,
    )
    gate_value, up_value = lax.psum((gate_part, up_part), "row")
    hidden = (jax.nn.silu(gate_value) * up_value).astype(BF16)
    down_full = lax.all_gather(down_weight, "rep", axis=1, tiled=True)
    branch_sum = lax.psum_scatter(
        jnp.dot(hidden, down_full, preferred_element_type=F32),
        "grid",
        scatter_dimension=0,
        tiled=True,
    )
    mixed = (tokens.astype(F32) + branch_sum).astype(BF16)
    held = lax.optimization_barrier(mixed).astype(F32)
    squares = lax.psum(jnp.sum(held * held, axis=1), "row")
    scale = lax.rsqrt(squares / width + 1e-05)
    normed = (held * scale[:, None] * norm_gain[None, :]).astype(BF16)
    partial_logits = jnp.dot(
        lax.all_gather(normed, ("grid", "rep"), axis=0, tiled=True),
        vocab_weight,
        preferred_element_type=F32,
    )
    logits = lax.psum(partial_logits, "row")
    block_index = lax.axis_index(("grid", "rep"))
    column_start = block_index * vocab_weight.shape[1]
    every_logprob = stats_all(logits, target_tokens, column_start)
    logprob = lax.dynamic_slice_in_dim(every_logprob, block_index * own_rows, own_rows, 0)
    return (mixed, logprob)


def tiles(width, tile=TILE):
    full = width // tile
    return full, width - full * tile


def over_tiles(width, step, tile=TILE):
    full, rest = tiles(width, tile)

    def one(n, carry):
        step(pl.ds(pl.multiple_of(n * tile, tile), tile))
        return carry

    if full == 1:
        step(pl.ds(0, tile))
    elif full:
        lax.fori_loop(0, full, one, 0)
    if rest:
        step(pl.ds(full * tile, rest))


class Sems:
    def __init__(self, send, recv):
        self.send, self.recv, self.used = send, recv, 0

    def take(self, count=1):
        first = self.used
        self.used += count
        return first


def block_kernel(
    tok_hbm, tgt_ref, gain_ref, wg_hbm, wu_hbm, wd_hbm, wv_hbm, mixed_hbm, lp_ref,
    WG, WU, WD, WV, TOKS, X, GU, RB, PS, PR, H, RSS, RSR, OWN, MX, NB, SQS, SQR, L, LR,
    TG, ST, SR, send_sem, recv_sem, local_sem,
):
    z = lax.axis_index("grid")
    r = lax.axis_index("row")
    p = lax.axis_index("rep")
    own_rows = tok_hbm.shape[0]
    wave_rows = own_rows // 2
    chunk = wave_rows * 2
    quarter = chunk // 4
    dc = wg_hbm.shape[0]
    ff = wg_hbm.shape[1]
    vocab = wv_hbm.shape[0]
    width = 4 * dc

    row_peer = {"grid": z, "row": 1 - r, "rep": p}
    x_peer = {"grid": z, "row": r, "rep": 1 - p}

    def pal(s):
        return (z, z + 1 - 2 * lax.rem(z, 2), lax.rem(z + 2, RING), RING - 1 - z)[s]

    near = 1 + lax.rem(z, 2)
    far = jnp.where(z < RING // 2, RING - 1, 0)
    inner = jnp.where(z < RING // 2, RING // 2, RING // 2 - 1)
    turn = (z, near, 6 - z - near - far, far)
    targets = (pal(1), inner, far)
    at_end = jnp.logical_or(z == 0, z == RING - 1)
    inside = jnp.logical_and(z > 0, z < RING - 1)

    def at_grid(there):
        return {"grid": there, "row": r, "rep": p}

    sems = Sems(send_sem, recv_sem)

    def remote(src, dst, sem, device, landing=None):
        landing = sem if landing is None else landing
        return pltpu.make_async_remote_copy(
            src_ref=src, dst_ref=dst, send_sem=send_sem.at[sem], recv_sem=recv_sem.at[landing],
            device_id=device, device_id_type=MESH,
        )

    def to_chip(block, sem, there):
        return remote(block, block, sem + there, at_grid(there), sem + z)

    open_sends = {}

    def send(src, dst, sem, device):
        copy = remote(src, dst, sem, device)
        copy.start()
        open_sends[sem] = copy

    def sent(sem):
        open_sends.pop(sem).wait_send()

    def arrived(dst, sem):
        remote(dst, dst, sem, row_peer).wait_recv()

    loads = []

    def load(src, dst, n):
        copy = pltpu.make_async_copy(src, dst, local_sem.at[n])
        copy.start()
        loads.append(copy)
        return copy

    tok_loads = []
    for w in range(2):
        rows = pl.ds(w * wave_rows, wave_rows)
        theirs = pl.ds(pl.multiple_of((1 - p) * dc, dc), dc)
        mine = pl.ds(pl.multiple_of(p * dc, dc), dc)
        tok_loads.append((
            load(tok_hbm.at[rows, theirs], TOKS.at[w], 2 * w),
            load(tok_hbm.at[rows, mine], X.at[z, w, p], 2 * w + 1),
        ))
    wg_load = load(wg_hbm, WG, 4)
    wu_load = load(wu_hbm, WU, 5)
    wd_load = load(wd_hbm, WD, 6)
    wv_load = load(wv_hbm, WV, 7)

    barrier = pltpu.get_barrier_semaphore()
    for s in range(RING):
        for dr in range(2):
            for dp in range(2):
                if s or dr or dp:
                    pl.semaphore_signal(
                        barrier, inc=1,
                        device_id={"grid": lax.rem(z + s, RING), "row": lax.rem(r + dr, 2), "rep": lax.rem(p + dp, 2)},
                        device_id_type=MESH,
                    )
    pl.semaphore_wait(barrier, 4 * RING - 1)

    tok_x = [sems.take() for _ in range(2)]
    tok_z = [sems.take(RING) for _ in range(2)]
    for w in range(2):
        tok_loads[w][0].wait()
        send(TOKS.at[w], X.at[z, w, p], tok_x[w], x_peer)

    def take_tokens(w):
        tok_loads[w][1].wait()
        arrived(X.at[z, w, 1 - p], tok_x[w])

    def tokens_to(w, n):
        return to_chip(X.at[z, w], tok_z[w], targets[n])

    def spread_tokens(w, from_middle, from_end):
        @pl.when(inside)
        def _():
            for n in from_middle:
                tokens_to(w, n).start()

        @pl.when(at_end)
        def _():
            for n in from_end:
                tokens_to(w, n).start()

    n_chunks = 2 * RING
    order = [(0, s) for s in range(RING)] + [(1, s) for s in (3, 1, 2, 0)]

    def ring(slots, make):
        made = [make() for _ in range(slots)]
        return [made[c % slots] for c in range(n_chunks)]

    dd = ring(2, lambda: [sems.take() for _ in range(2)])
    xp = ring(4, lambda: [sems.take() for _ in range(2)])
    xh = ring(4, sems.take)
    dh = ring(4, sems.take)
    df = ring(4, sems.take)
    rs = [sems.take(RING) for _ in range(2)]

    def gate_up(c):
        w, s = order[c]
        zo = turn[s]
        slot = c % 2
        if s:
            arrived(X.at[zo, w], tok_z[w] + zo)
        for g, weight in enumerate((WG, WU)):
            if c >= 2:
                sent(dd[c - 2][g])

            def step(cols):
                x = X[zo, w].reshape(chunk, dc)
                part = jnp.dot(x, weight[:, cols], preferred_element_type=F32)
                for a in range(2):
                    for b in range(2):
                        at = (2 * a + b) * quarter
                        GU[slot, a, g, b, :, cols] = part[at : at + quarter]

            over_tiles(ff, step, GATE_TILE)
            send(GU.at[slot, 1 - r, g], RB.at[slot, g], dd[c][g], row_peer)

    def sum_rows(c):
        slot = c % 2
        if c >= 4:
            sent(df[c - 4])
        for g in range(2):
            if c >= 2:
                sent(xp[c - 2][g])
            arrived(RB.at[slot, g], dd[c][g])

            def step(cols):
                PS[slot, g, :, cols] = (
                    GU[slot, r, g, 1 - p, :, cols] + RB[slot, g, 1 - p, :, cols]
                ).astype(BF16)
                GU[slot, r, g, p, :, cols] = GU[slot, r, g, p, :, cols] + RB[slot, g, p, :, cols]

            over_tiles(ff, step)
            send(PS.at[slot, g], PR.at[c % 4, g], xp[c][g], x_peer)

    def activate(c):
        slot = c % 2
        hs = c % 4
        for g in range(2):
            arrived(PR.at[hs, g], xp[c][g])
        if c >= 4:
            sent(xh[c - 4])
            sent(dh[c - 4])

        def step(cols):
            gate = GU[slot, r, 0, p, :, cols] + PR[hs, 0, :, cols].astype(F32)
            up_value = GU[slot, r, 1, p, :, cols] + PR[hs, 1, :, cols].astype(F32)
            hidden = gate / (1.0 + jnp.exp(-gate)) * up_value
            H[hs, r, p, :, cols] = hidden.astype(BF16)

        over_tiles(ff, step)
        send(H.at[hs, r, p], H.at[hs, r, p], xh[c], x_peer)
        send(H.at[hs, r, p], H.at[hs, r, p], dh[c], row_peer)

    def pass_on(c):
        hs = c % 4
        arrived(H.at[hs, r, 1 - p], xh[c])
        send(H.at[hs, r, 1 - p], H.at[hs, r, 1 - p], df[c], row_peer)

    def project(c):
        w, s = order[c]
        hs = c % 4
        arrived(H.at[hs, 1 - r, p], dh[c])
        arrived(H.at[hs, 1 - r, 1 - p], df[c])

        def step(cols):
            h = H[hs].reshape(chunk, ff)
            part = jnp.dot(h, WD[:, cols], preferred_element_type=F32)
            if s:
                RSS[w, s - 1, :, cols] = part.astype(BF16)
            else:
                OWN[w, :, cols] = part

        over_tiles(dc, step, PROJECT_TILE)
        if s:
            there = turn[s]
            copy = remote(RSS.at[w, s - 1], RSR.at[w, z], rs[w] + there, at_grid(there), rs[w] + z)
            copy.start()
            open_sends["sums", w, s] = copy

    def finish_rows(w):
        for there in turn[1:]:
            arrived(RSR.at[w, there], rs[w] + there)

        def step(cols):
            total = OWN[w, :, cols]
            for there in turn[1:]:
                total = total + RSR[w, there, :, cols].astype(F32)
            own = X[z, w, :, :, cols].reshape(chunk, cols.size).astype(F32)
            MX[z, w, p, :, cols] = (own + total).astype(BF16)

        over_tiles(dc, step)

    gz = [sems.take(RING) for _ in range(2)]
    hk = [sems.take(2) for _ in range(2)]
    gx = [[sems.take() for _ in range(RING)] for _ in range(2)]

    def gather_z(w, there):
        return to_chip(MX.at[z, w, p], gz[w], there)

    def start_gather(w):
        for there in targets[:2]:
            gather_z(w, there).start()

    def outward(w, n):
        zb = targets[n]
        block = MX.at[zb, w, p]
        return remote(block, block, hk[w] + n - 1, at_grid(pal(1)), gz[w] + zb)

    def hand_on(w, n):
        @pl.when(inside)
        def _():
            arrived(MX.at[targets[n], w, p], gz[w] + targets[n])
            outward(w, n).start()

    def drain_gather(w):
        for there in targets[:2]:
            gather_z(w, there).wait_send()

        @pl.when(inside)
        def _():
            for n in (1, 2):
                outward(w, n).wait_send()

    def begin_first(ready):
        @pl.when(ready)
        def _():
            finish_rows(0)
            start_gather(0)

    def share(w, n, when_inside=True, when_at_end=True):
        zb = sources[n]
        block = MX.at[zb, w, p]
        copy = remote(block, block, gx[w][n], x_peer)
        open_sends["share", w, n] = copy
        if n < 2:
            if n == 1:
                arrived(block, gz[w] + zb)
            copy.start()
            return
        if when_inside:

            @pl.when(inside)
            def _():
                copy.start()

        if when_at_end:

            @pl.when(at_end)
            def _():
                arrived(block, gz[w] + zb)
                copy.start()

    def shared(w, n):
        arrived(MX.at[sources[n], w, 1 - p], gx[w][n])

    sources = (z,) + targets

    take_tokens(0)
    spread_tokens(0, (0, 1), ())
    wg_load.wait()
    wu_load.wait()
    gate_up(0)
    spread_tokens(0, (2,), (0,))
    sum_rows(0)
    gate_up(1)
    spread_tokens(0, (), (1, 2))
    sum_rows(1)
    take_tokens(1)
    for i in range(n_chunks + 1):
        if i < n_chunks:
            activate(i)
        if i == n_chunks - 2:
            hand_on(0, 1)
        if i == n_chunks - 1:
            share(0, 0)
        if i + 2 < n_chunks:
            gate_up(i + 2)
        if i >= 1:
            pass_on(i - 1)
        if i + 2 < n_chunks:
            sum_rows(i + 2)
        if i == 1:
            wd_load.wait()
        if i >= 1:
            project(i - 1)
        if i == n_chunks - 1:
            share(0, 1)
            hand_on(0, 2)
        if i == 0:
            spread_tokens(1, (2, 1), (2, 1))
        if i == 1:
            spread_tokens(1, (0,), (0,))
        if i == 4:
            begin_first(inside)
        if i == 6:
            begin_first(at_end)
    finish_rows(1)
    start_gather(1)
    share(0, 2)
    share(1, 0)
    share(0, 3)

    sq = [sems.take() for _ in range(n_chunks)]
    lg = [[sems.take(2) for _ in range(2)] for _ in range(2)]
    half = vocab // 2
    rows_tile = max(t for t in range(16, TILE + 1, 16) if half % t == 0)
    hop = half // 32 * 16
    big_tile = half - hop
    here = lax.div(z, 2)

    def squares(k, zb, w):
        def part(h):
            v = MX[zb, w, h].astype(F32)
            return jnp.sum(v * v, axis=1, keepdims=True)

        SQS[k] = jnp.broadcast_to(part(0) + part(1), (chunk, LANES))
        send(SQS.at[k], SQR.at[k], sq[k], row_peer)

    def normalise(k, zb, w):
        arrived(SQR.at[k], sq[k])
        scale = lax.rsqrt((SQS[k] + SQR[k])[:, :1] / width + 1e-05)
        for h in range(2):
            cols = slice(h * dc, (h + 1) * dc)
            v = MX[zb, w, h].astype(F32) * scale * gain_ref[:, cols]
            NB[lax.div(zb, 2), lax.rem(zb, 2), :, cols] = v.astype(BF16)

    def logits_half(side, first_tile=0, last_tile=2):
        def step(n, carry):
            at = pl.multiple_of(n * hop, 16)
            rows = pl.ds(pl.multiple_of(side * half + at, 16), big_tile)
            x = NB[...].reshape(-1, 2 * dc)
            part = lax.dot_general(
                WV[rows, :], x, (((1,), (1,)), ((), ())), preferred_element_type=F32
            )
            for g in range(2):
                L[g, side, pl.ds(at, big_tile)] = part[:, g * LANES : (g + 1) * LANES]
            return carry

        lax.fori_loop(first_tile, last_tile, step, 0)

    def exchange(w, piece):
        rows = (pl.ds(0, hop), pl.ds(hop, big_tile))[piece]
        for g in range(2):
            send(L.at[g, 1 - r, rows], LR.at[w, g, rows], lg[w][g] + piece, row_peer)

    row_start = (z * 2 + p) * vocab + r * half

    def stats(w, group):
        arrived(LR.at[w, group, pl.ds(0, hop)], lg[w][group])
        arrived(LR.at[w, group, pl.ds(hop, big_tile)], lg[w][group] + 1)
        step_rows = rows_tile
        steps = half // step_rows

        def add(i, top):
            rows = pl.ds(pl.multiple_of(i * step_rows, 8), step_rows)
            t = L[group, r, rows] + LR[w, group, rows]
            L[group, r, rows] = t
            return jnp.maximum(top, jnp.max(t.reshape(-1, 8, LANES), axis=0))

        top = lax.fori_loop(0, steps, add, jnp.full((8, LANES), -jnp.inf, F32))
        top = jnp.max(top, axis=0, keepdims=True)
        target = TG[w, group, 0:1] - row_start

        def count(i, carry):
            total, picked = carry
            rows = pl.ds(pl.multiple_of(i * step_rows, 8), step_rows)
            t = L[group, r, rows]
            ids = lax.broadcasted_iota(jnp.int32, t.shape, 0) + i * step_rows
            e = jnp.exp(t - top)
            hit = jnp.where(ids == target, t, 0.0)
            return (
                total + jnp.sum(e.reshape(-1, 8, LANES), axis=0),
                picked + jnp.sum(hit.reshape(-1, 8, LANES), axis=0),
            )

        zero = jnp.zeros((8, LANES), F32)
        total, picked = lax.fori_loop(0, steps, count, (zero, zero))
        ST[group, 4 * w : 4 * w + 1] = top
        ST[group, 4 * w + 1 : 4 * w + 2] = jnp.sum(total, axis=0, keepdims=True)
        ST[group, 4 * w + 2 : 4 * w + 3] = jnp.sum(picked, axis=0, keepdims=True)

    lane = lax.broadcasted_iota(jnp.int32, (8, LANES), 1)
    ST[...] = jnp.zeros_like(ST)
    for g in range(2):
        for w in range(2):
            line = None
            for spot in range(4):
                source = 2 * (spot % 2) + w
                ids = jnp.broadcast_to(tgt_ref[2 * g + spot // 2], (8, LANES))
                ids = pltpu.roll(ids, ((spot - source) * wave_rows) % LANES, 1)
                line = ids if line is None else jnp.where(lane >= spot * wave_rows, ids, line)
            TG[w, g] = line

    for n in range(RING):
        shared(0, n)
        squares(n, sources[n], 0)
        if n == 1:
            share(1, 1)
        if n == 2:
            hand_on(1, 1)
            share(1, 2, when_at_end=False)
            hand_on(1, 2)
            share(1, 3, when_at_end=False)
    wv_load.wait()
    for n in range(RING):
        normalise(n, sources[n], 0)
    logits_half(1 - r)
    exchange(0, 0)
    exchange(0, 1)
    share(1, 2, when_inside=False)
    share(1, 3, when_inside=False)
    logits_half(r)
    for n in range(2):
        shared(1, n)
        squares(RING + n, sources[n], 1)
    outs = []
    for w in range(2):
        for h in range(2):
            rows = pl.ds(pl.multiple_of(p * wave_rows, wave_rows), wave_rows)
            copy = pltpu.make_async_copy(
                MX.at[z, w, h, rows],
                mixed_hbm.at[pl.ds(w * wave_rows, wave_rows), pl.ds(h * dc, dc)],
                local_sem.at[2 * w + h],
            )
            copy.start()
            outs.append(copy)

    for g in range(2):
        stats(0, g)
    for g in range(2):
        for piece in range(2):
            sent(lg[0][g] + piece)
    for n in (2, 3):
        shared(1, n)
        squares(RING + n, sources[n], 1)
    for n in range(RING):
        normalise(RING + n, sources[n], 1)
    for piece in range(2):
        logits_half(1 - r, piece, piece + 1)
        exchange(1, piece)
    logits_half(r)
    for g in range(2):
        stats(1, g)

    n_all = 4 * RING
    base = sems.take(n_all)
    assert sems.used <= N_SEMS, sems.used
    me = (z * 2 + r) * 2 + p

    def others():
        for s in (3, 2, 1, 0):
            for dr in range(2):
                for dp in range(2):
                    if s or dr or dp:
                        yield s, dr, dp

    def figures(s, dr, dp):
        device = {"grid": pal(s), "row": lax.rem(r + dr, 2), "rep": lax.rem(p + dp, 2)}
        return pltpu.make_async_remote_copy(
            src_ref=ST.at[lax.div(pal(s), 2)], dst_ref=SR.at[me],
            send_sem=send_sem.at[base + 4 * s + 2 * dr + dp], recv_sem=recv_sem.at[base + me],
            device_id=device, device_id_type=MESH,
        )

    for other in others():
        figures(*other).start()
    SR[me] = ST[here]
    for s, dr, dp in others():
        who = (pal(s) * 2 + lax.rem(r + dr, 2)) * 2 + lax.rem(p + dp, 2)
        arrived(SR.at[who], base + who)

    lines = []
    for w in range(2):
        top = SR[0, 4 * w : 4 * w + 1]
        for n in range(1, n_all):
            top = jnp.maximum(top, SR[n, 4 * w : 4 * w + 1])
        total = jnp.zeros_like(top)
        picked = jnp.zeros_like(top)
        for n in range(n_all):
            total = total + SR[n, 4 * w + 1 : 4 * w + 2] * jnp.exp(SR[n, 4 * w : 4 * w + 1] - top)
            picked = picked + SR[n, 4 * w + 2 : 4 * w + 3]
        lines.append(jnp.broadcast_to(picked - top - jnp.log(total), (8, LANES)))
    spot = lax.rem(z, 2) * 2 + p
    result = jnp.zeros((8, LANES), F32)
    for k in range(4):
        a = pltpu.roll(lines[0], (-k * wave_rows) % LANES, 1)
        b = pltpu.roll(lines[1], ((1 - k) * wave_rows) % LANES, 1)
        result = jnp.where(spot == k, jnp.where(lane < wave_rows, a, b), result)
    lp_ref[...] = result[0:1, : lp_ref.shape[1]]

    for other in others():
        figures(*other).wait_send()
    for w in range(2):
        for n in range(3):
            tokens_to(w, n).wait_send()
        drain_gather(w)
    for sem in list(open_sends):
        sent(sem)
    for copy in outs:
        copy.wait()


N_SEMS = 96


def hand_over(mixed_ref, lp_ref, mixed_out, lp_out):
    mixed_out[...] = mixed_ref[...]
    lp_out[...] = lp_ref[...]


def block(tokens, target_tokens, gate_weight, up_weight, down_weight, norm_gain, vocab_weight):
    own_rows, half_width = tokens.shape
    wave_rows = own_rows // 2
    chunk = 2 * wave_rows
    quarter = chunk // 4
    dc, ff = gate_weight.shape
    vocab = vocab_weight.shape[1]
    vmem = pltpu.VMEM
    any_space = pl.BlockSpec(memory_space=pl.ANY)
    in_vmem = pl.BlockSpec(memory_space=pltpu.VMEM)
    targets = target_tokens.reshape(RING, 1, 2 * own_rows)
    gain = norm_gain.reshape(1, half_width)
    mixed, logprob = pl.pallas_call(
        block_kernel,
        out_shape=(
            jax.ShapeDtypeStruct((own_rows, half_width), BF16),
            jax.ShapeDtypeStruct((1, own_rows), F32),
        ),
        in_specs=[any_space, in_vmem, in_vmem, any_space, any_space, any_space, any_space],
        out_specs=(any_space, in_vmem),
        scratch_shapes=[
            vmem((dc, ff), BF16),
            vmem((dc, ff), BF16),
            vmem((ff, dc), BF16),
            vmem((vocab, half_width), BF16),
            vmem((2, wave_rows, dc), BF16),
            vmem((RING, 2, 2, wave_rows, dc), BF16),
            vmem((2, 2, 2, 2, quarter, ff), F32),
            vmem((2, 2, 2, quarter, ff), F32),
            vmem((2, 2, quarter, ff), BF16),
            vmem((4, 2, quarter, ff), BF16),
            vmem((4, 2, 2, quarter, ff), BF16),
            vmem((2, RING - 1, chunk, dc), BF16),
            vmem((2, RING, chunk, dc), BF16),
            vmem((2, chunk, dc), F32),
            vmem((RING, 2, 2, chunk, dc), BF16),
            vmem((2, 2, chunk, half_width), BF16),
            vmem((2 * RING, chunk, LANES), F32),
            vmem((2 * RING, chunk, LANES), F32),
            vmem((2, 2, vocab // 2, LANES), F32),
            vmem((2, 2, vocab // 2, LANES), F32),
            vmem((2, 2, 8, LANES), jnp.int32),
            vmem((2, 8, LANES), F32),
            vmem((4 * RING, 8, LANES), F32),
            pltpu.SemaphoreType.DMA((N_SEMS,)),
            pltpu.SemaphoreType.DMA((N_SEMS,)),
            pltpu.SemaphoreType.DMA((8,)),
        ],
        compiler_params=pltpu.CompilerParams(
            collective_id=0, has_side_effects=True, vmem_limit_bytes=67_043_328
        ),
        name="block",
    )(tokens, targets, gain, gate_weight, up_weight, down_weight, vocab_weight.T)
    mixed, logprob = pl.pallas_call(
        hand_over,
        out_shape=(
            jax.ShapeDtypeStruct((own_rows, half_width), BF16),
            jax.ShapeDtypeStruct((1, own_rows), F32),
        ),
        in_specs=[in_vmem, in_vmem],
        out_specs=(in_vmem, in_vmem),
        name="hand_over",
    )(mixed, logprob)
    return (mixed, logprob.reshape(own_rows))


def solution(mesh):
    in_specs = (
        P(("groups", "grid", "rep"), "row"),
        P("groups"),
        P(("row", "rep"), "grid"),
        P(("row", "rep"), "grid"),
        P("grid", ("row", "rep")),
        P("row"),
        P("row", ("grid", "rep")),
    )
    out_specs = (P(("groups", "grid", "rep"), "row"), P(("groups", "grid", "rep")))
    small = mesh.shape["row"] == 2 and mesh.shape["rep"] == 2 and mesh.shape["grid"] == RING
    return jax.shard_map(
        block if small else general,
        mesh=mesh,
        in_specs=in_specs,
        out_specs=out_specs,
        check_vma=False,
    )
```
